32 devices in a mesh: dp: 8 (over z, y), tensor: 4 (over x, core).
Axes of the slice: x: 2, y: 2, z: 4, core: 2. Of those that a mesh axis runs over, the one named last changes fastest.
Arguments:
- tokens: bfloat16 [12288, 1024], P('dp', 'tensor'), may hold values from -6 to 6
- segment_ids: int32 [12288], P('dp'), may hold values from 0 to 8, as said below
- w_query: bfloat16 [1024, 1024], P(None, 'tensor'), may hold values from -0.1875 to 0.1875
- w_key: bfloat16 [1024, 1024], P(None, 'tensor'), may hold values from -0.1875 to 0.1875
- w_value: bfloat16 [1024, 1024], P(None, 'tensor'), may hold values from -0.1875 to 0.1875
- b_query: bfloat16 [1024], P('tensor'), may hold values from -3 to 3
- b_value: bfloat16 [1024], P('tensor'), may hold values from -3 to 3
- w_out: bfloat16 [1024, 1024], P('tensor'), may hold values from -0.75 to 0.75
- b_out: bfloat16 [1024], P('tensor'), may hold values from -3 to 3
- gain_one: bfloat16 [1024], P('tensor'), may hold values from 0.5 to 1.5
- bias_one: bfloat16 [1024], P('tensor'), may hold values from -3 to 3
- w_in: bfloat16 [1024, 4096], P(None, 'tensor'), may hold values from -0.1875 to 0.1875
- b_in: bfloat16 [4096], P('tensor'), may hold values from -3 to 3
- w_down: bfloat16 [4096, 1024], P('tensor'), may hold values from -0.09375 to 0.09375
- b_down: bfloat16 [1024], P('tensor'), may hold values from -3 to 3
- gain_two: bfloat16 [1024], P('tensor'), may hold values from 0.5 to 1.5
- bias_two: bfloat16 [1024], P('tensor'), may hold values from -3 to 3
- cotangent: bfloat16 [12288, 1024], P('dp', 'tensor'), may hold values from -6 to 6
Outputs:
- out: bfloat16 [12288, 1024], P('dp', 'tensor')
- grad_tokens: bfloat16 [12288, 1024], P('dp', 'tensor')
- grad_w_query: float32 [1024, 1024], P(None, 'tensor')
- grad_w_key: float32 [1024, 1024], P(None, 'tensor')
- grad_w_value: float32 [1024, 1024], P(None, 'tensor')
- grad_b_query: float32 [1024], P('tensor')
- grad_b_value: float32 [1024], P('tensor')
- grad_w_out: float32 [1024, 1024], P('tensor')
- grad_b_out: float32 [1024], P('tensor')
- grad_gain_one: float32 [1024], P('tensor')
- grad_bias_one: float32 [1024], P('tensor')
- grad_w_in: float32 [1024, 4096], P(None, 'tensor')
- grad_b_in: float32 [4096], P('tensor')
- grad_w_down: float32 [4096, 1024], P('tensor')
- grad_b_down: float32 [1024], P('tensor')
- grad_gain_two: float32 [1024], P('tensor')
- grad_bias_two: float32 [1024], P('tensor')
The draws below stay inside these ranges and needn't reach their ends.
Inputs may be any that keep to these rules, and one draw needn't show every extreme that they name: `segment_ids`: within each packed sequence of 512 tokens the ids run from 1 to 8 without falling, each id on at least one token, followed by one or more tail slots of id 0.
All inputs are finite; a program needn't handle non-finite values.
Results may differ from the reference program's by a relative error of at most 0.015.
Values may be sent and summed in bfloat16 or wider, within the bound.
No kernel may reach another device: no remote copies, remote signals or barrier semaphores. Data moves between devices by JAX's collectives and lax.ppermute only.
A program may use at most 128 MiB of HBM per device.

```python
import jax
import jax.numpy as jnp
from jax import lax

D = 1024
H = 16
HD = 64
FF = 4096
LEN = 512
SEGS = 8
SEQS = 24
TOKENS = 12288


def one_sequence(key):
    length_key, tail_key = jax.random.split(key)
    powers = jax.random.randint(length_key, (SEGS,), 0, 5)
    weights = jnp.power(2, powers).astype(jnp.int32)
    running = jnp.cumsum(weights)
    weight_total = running[SEGS - 1]
    used_slots = LEN - jax.random.randint(tail_key, (), 1, LEN // 4 + 1)
    bounds = jnp.arange(1, SEGS + 1, dtype=jnp.int32) + running * (used_slots - SEGS) // weight_total
    position = jnp.arange(LEN, dtype=jnp.int32)
    segment = 1 + jnp.sum((position[:, None] >= bounds[None, :SEGS - 1]).astype(jnp.int32), axis=1)
    return jnp.where(position < used_slots, segment, 0).astype(jnp.int32)


def draw_segment_ids(key, part):
    seq_keys = jax.random.split(key, SEQS)
    return jax.vmap(one_sequence)(seq_keys).reshape(SEQS * LEN)


def block_levels(stream_key, dims, cuts, least, largest):
    loudness = 1.0
    for dim, parts in cuts:
        draws = jax.random.uniform(jax.random.fold_in(jax.random.fold_in(stream_key, 6), dim), (parts,), jnp.float32, least / len(cuts), largest / len(cuts))
        loudness = loudness * jnp.repeat(jnp.exp(draws), dims[dim] // parts).reshape((-1,) + (1,) * (len(dims) - 1 - dim))
    return loudness


def noise(stream_key, shape, scale, reach, cuts=(), kind=jnp.bfloat16):
    loudness = block_levels(stream_key, shape, cuts, -0.22, 0.18) if cuts else 1.0
    values = jax.random.normal(stream_key, shape, jnp.float32) * scale * loudness
    return jnp.minimum(jnp.maximum(values, -reach), reach).astype(kind)


def setup_inputs(seed: int = 0) -> dict:
    seeds = jax.random.split(jax.random.key(seed), 19)
    return {
        "tokens": noise(seeds[0], (TOKENS, D), 1.0, 6.0, ((0, 8), (1, 4))),
        "segment_ids": draw_segment_ids(jax.random.fold_in(seeds[18], 71), 0),
        "w_query": noise(seeds[2], (D, D), D ** -0.5, 0.1875, ((1, 4),)),
        "w_key": noise(seeds[3], (D, D), D ** -0.5, 0.1875, ((1, 4),)),
        "w_value": noise(seeds[4], (D, D), D ** -0.5, 0.1875, ((1, 4),)),
        "b_query": noise(seeds[5], (D,), 0.5, 3.0, ((0, 4),)),
        "b_value": noise(seeds[6], (D,), 0.5, 3.0, ((0, 4),)),
        "w_out": noise(seeds[7], (D, D), (D // 16) ** -0.5, 0.75, ((0, 4),)),
        "b_out": noise(seeds[8], (D,), 0.5, 3.0, ((0, 4),)),
        "gain_one": jnp.clip(1.0 + 0.1 * jax.random.normal(seeds[9], (D,), jnp.float32), 0.5, 1.5).astype(jnp.bfloat16),
        "bias_one": noise(seeds[10], (D,), 0.5, 3.0, ((0, 4),)),
        "w_in": noise(seeds[11], (D, FF), D ** -0.5, 0.1875, ((1, 4),)),
        "b_in": noise(seeds[12], (FF,), 0.5, 3.0, ((0, 4),)),
        "w_down": noise(seeds[13], (FF, D), FF ** -0.5, 0.09375, ((0, 4),)),
        "b_down": noise(seeds[14], (D,), 0.5, 3.0, ((0, 4),)),
        "gain_two": jnp.clip(1.0 + 0.1 * jax.random.normal(seeds[15], (D,), jnp.float32), 0.5, 1.5).astype(jnp.bfloat16),
        "bias_two": noise(seeds[16], (D,), 0.5, 3.0, ((0, 4),)),
        "cotangent": noise(seeds[17], (TOKENS, D), 1.0, 6.0, ((0, 8), (1, 4))),
    }


epsilon = 1e-05
masked_fill = -1000000000.0

@jax.custom_vjp
def low(v):
    return lax.optimization_barrier(v.astype(jnp.bfloat16)).astype(jnp.float32)

@jax.custom_vjp
def low_back(v):
    return v

def low_keep(v):
    return (low(v), None)

def low_pass(kept, grad):
    return (grad,)

def back_keep(v):
    return (v, None)

def back_low(kept, grad):
    return (low(grad),)
low.defvjp(low_keep, low_pass)
low_back.defvjp(back_keep, back_low)

def matmul(left, right):
    return jnp.dot(left, right, precision=lax.Precision.HIGHEST, preferred_element_type=jnp.float32)

def layer_norm(values, gain_vec, shift_vec):
    center = values - lax.optimization_barrier(jnp.mean(values, axis=-1, keepdims=True))
    variance = lax.optimization_barrier(jnp.mean(center * center, axis=-1, keepdims=True))
    return center * lax.rsqrt(variance + epsilon) * gain_vec + shift_vec

def allowed_pairs(labels):
    length = labels.shape[-1]
    same_label = labels[..., :, None] == labels[..., None, :]
    diagonal = jnp.arange(length)[:, None] == jnp.arange(length)[None, :]
    return same_label & ((labels[..., :, None] != 0) | diagonal)

def attend(queries, key_proj, value_proj, labels):
    score_scale = HD ** (-0.5)
    scores = jnp.einsum('gqhd,gkhd->ghqk', queries, key_proj, precision=lax.Precision.HIGHEST) * score_scale
    scores = low_back(scores)
    scores = jnp.where(allowed_pairs(labels)[:, None], scores, masked_fill)
    probs = low(jax.nn.softmax(scores, axis=-1))
    return jnp.einsum('ghqk,gkhd->gqhd', probs, value_proj, precision=lax.Precision.HIGHEST)

def encoder_layer(inputs, labels, w_query, w_key, w_value, b_query, b_value, w_out, b_out, gain_one, bias_one, w_in, b_in, w_down, b_down, gain_two, bias_two):
    seq_count = labels.shape[0]

    def heads_of(values):
        return low(low_back(values)).reshape(seq_count, LEN, H, HD)
    queries = heads_of(matmul(inputs, w_query) + b_query)
    key_proj = heads_of(matmul(inputs, w_key))
    value_proj = heads_of(matmul(inputs, w_value) + b_value)
    context = attend(queries, key_proj, value_proj, labels).reshape(seq_count * LEN, D)
    context = low(low_back(context))
    z_one = inputs + low_back(matmul(context, w_out)) + b_out
    h_one = layer_norm(z_one, gain_one, bias_one)
    h_low = low(h_one)
    pre_act = low_back(matmul(h_low, w_in) + b_in)
    hidden = low(jax.nn.gelu(pre_act, approximate=False))
    z_two = h_one + low_back(matmul(hidden, w_down)) + b_down
    return layer_norm(z_two, gain_two, bias_two)

def reference(tokens, segment_ids, w_query, w_key, w_value, b_query, b_value, w_out, b_out, gain_one, bias_one, w_in, b_in, w_down, b_down, gain_two, bias_two, cotangent):
    params = tuple((weight.astype(jnp.float32) for weight in (w_query, w_key, w_value, b_query, b_value, w_out, b_out, gain_one, bias_one, w_in, b_in, w_down, b_down, gain_two, bias_two)))
    batch_seqs = 4
    groups = TOKENS // (batch_seqs * LEN)
    inputs = tokens.astype(jnp.float32).reshape(groups, batch_seqs * LEN, D)
    labels = segment_ids.astype(jnp.int32).reshape(groups, batch_seqs, LEN)
    cotans = cotangent.astype(jnp.float32).reshape(groups, batch_seqs * LEN, D)
    starting = tuple((jnp.zeros_like(weight) for weight in params))

    def group_step(totals, sliced):
        rows_in, labels_in, cotan_in = sliced

        def forward(x_rows, *weights):
            return encoder_layer(x_rows, labels_in, *weights)
        result, pull = jax.vjp(forward, rows_in, *params)
        grads = pull(cotan_in)
        totals = tuple((left + right for left, right in zip(totals, grads[1:])))
        return (totals, (result.astype(jnp.bfloat16), grads[0].astype(jnp.bfloat16)))
    totals, (results, input_grads) = lax.scan(group_step, starting, (inputs, labels, cotans))
    return (results.reshape(TOKENS, D), input_grads.reshape(TOKENS, D), totals[0], totals[1], totals[2], totals[3], totals[4], totals[5], totals[6], totals[7], totals[8], totals[9], totals[10], totals[11], totals[12], totals[13], totals[14])
```

```python
import functools
import math

import jax
import jax.numpy as jnp
from jax import lax
from jax.experimental import pallas as pl
from jax.experimental.pallas import tpu as pltpu
from jax.sharding import PartitionSpec as P

HD = 64
LEN = 512
CHUNKS = (1, 1, 1)

EPSILON = 1e-05
MASKED = -1000000000.0
BF = jnp.bfloat16
F32 = jnp.float32


def mm(left, right):
    return lax.dot_general(left, right, (((1,), (0,)), ((), ())), preferred_element_type=F32)


def over_rows(left, right):
    return lax.dot_general(left, right, (((0,), (0,)), ((), ())), preferred_element_type=F32)


def against(left, right):
    return lax.dot_general(left, right, (((1,), (1,)), ((), ())), preferred_element_type=F32)


def swap(values, axis, bit):
    size = lax.axis_size(axis)
    return lax.ppermute(values, axis, [(i, i ^ bit) for i in range(size)])


def xor_order(blocks, t):
    odd = (t & 1) == 1
    upper = (t & 2) == 2
    b0, b1, b2, b3 = blocks
    q0, q1 = jnp.where(odd, b1, b0), jnp.where(odd, b0, b1)
    q2, q3 = jnp.where(odd, b3, b2), jnp.where(odd, b2, b3)
    return (
        jnp.where(upper, q2, q0),
        jnp.where(upper, q3, q1),
        jnp.where(upper, q0, q2),
        jnp.where(upper, q1, q3),
    )


def gather_blocks(own):
    across = swap(own, "tensor", 2)
    beside = swap(own, "tensor", 1)
    corner = swap(across, "tensor", 1)
    return own, beside, across, corner


def exchange_blocks(blocks):
    return (
        blocks[0],
        swap(blocks[1], "tensor", 1),
        swap(blocks[2], "tensor", 2),
        swap(blocks[3], "tensor", 3),
    )


def scatter_sum(blocks):
    b0, b1, b2, b3 = blocks
    far = swap(b3, "tensor", 1)
    near = swap(b1, "tensor", 1)
    onward = (b2.astype(F32) + far.astype(F32)).astype(BF)
    across = swap(onward, "tensor", 2)
    return (b0.astype(F32) + near.astype(F32)) + across.astype(F32)


def reduce_rows(values, bits, index):
    for bit in bits:
        half = values.shape[0] // 2
        mine = jnp.where((index & bit) == 0, 0, half)
        sent = lax.dynamic_slice_in_dim(values, half - mine, half, 0).astype(BF)
        kept = lax.dynamic_slice_in_dim(values, mine, half, 0)
        got = swap(sent, "dp", bit)
        values = kept.astype(F32) + got.astype(F32)
    return values.astype(BF)


def spread_rows(values, bits, index):
    for bit in reversed(bits):
        got = swap(values, "dp", bit)
        low = (index & bit) == 0
        values = jnp.concatenate([jnp.where(low, values, got), jnp.where(low, got, values)], axis=0)
    return values


def dp_bits(order):
    size = lax.axis_size("dp")
    bits = [1 << i for i in range(int(math.log2(size)))]
    turn = order % len(bits)
    return bits[turn:] + bits[:turn]


def summed_big(values, order, index):
    bits = dp_bits(order)
    return spread_rows(reduce_rows(values, bits, index), bits, index).astype(F32)


def summed_small(values):
    for bit in dp_bits(0):
        values = values + swap(values, "dp", bit)
    return values


def head_lanes(width, head):
    lane = lax.broadcasted_iota(jnp.int32, (1, width), 1)
    return (lane >= head * HD) & (lane < (head + 1) * HD)


def allowed_block(row_labels, column_labels):
    length = row_labels.shape[0]
    same = row_labels == column_labels
    diagonal = lax.broadcasted_iota(jnp.int32, (length, length), 0) == lax.broadcasted_iota(
        jnp.int32, (length, length), 1
    )
    return same & ((row_labels != 0) | diagonal)


def attend_kernel(q_ref, k_ref, v_ref, rows_ref, columns_ref, context_ref, total_ref):
    width = q_ref.shape[1]
    allowed = allowed_block(rows_ref[0], columns_ref[0])
    queries, keys, values = q_ref[...], k_ref[...], v_ref[...]
    context = jnp.zeros(q_ref.shape, F32)
    zero = jnp.zeros((), BF)
    for head in range(width // HD):
        lanes = head_lanes(width, head)
        scores = against(jnp.where(lanes, queries, zero), keys) * (HD**-0.5)
        scores = jnp.where(allowed, scores, MASKED)
        peak = jnp.max(scores, axis=1, keepdims=True)
        terms = jnp.exp(scores - peak)
        total = jnp.sum(terms, axis=1, keepdims=True)
        probs = (terms / total).astype(BF)
        context = context + mm(probs, jnp.where(lanes, values, zero))
        total_ref[0, :, head : head + 1] = peak + jnp.log(total)
    context_ref[...] = context.astype(BF)


def attend_back_kernel(
    q_ref, k_ref, v_ref, rows_ref, columns_ref, dcontext_ref, total_ref, out_ref
):
    width = q_ref.shape[1]
    allowed = allowed_block(rows_ref[0], columns_ref[0])
    queries, keys, values = q_ref[...], k_ref[...], v_ref[...]
    dcontext = dcontext_ref[...]
    scale = HD**-0.5
    dquery = jnp.zeros(q_ref.shape, F32)
    dkey = jnp.zeros(q_ref.shape, F32)
    dvalue = jnp.zeros(q_ref.shape, F32)
    zero = jnp.zeros((), BF)
    for head in range(width // HD):
        lanes = head_lanes(width, head)
        q_head = jnp.where(lanes, queries, zero)
        d_head = jnp.where(lanes, dcontext, zero)
        k_head = jnp.where(lanes, keys, zero)
        scores = against(q_head, keys) * scale
        scores = jnp.where(allowed, scores, MASKED)
        probs = jnp.exp(scores - total_ref[0, :, head : head + 1])
        dprobs = against(d_head, values)
        delta = jnp.sum(probs * dprobs, axis=1, keepdims=True)
        dscores = (probs * (dprobs - delta)).astype(BF)
        dquery = dquery + mm(dscores, k_head)
        dkey = dkey + over_rows(dscores, q_head)
        dvalue = dvalue + over_rows(probs.astype(BF), d_head)
    out_ref[:, :width] = (dquery * scale).astype(BF)
    out_ref[:, width : 2 * width] = (dkey * scale).astype(BF)
    out_ref[:, 2 * width :] = dvalue.astype(BF)


def sequence_specs(width):
    def third(part):
        return pl.BlockSpec((LEN, width), lambda s: (s, part))

    return [
        third(0),
        third(1),
        third(2),
        pl.BlockSpec((1, LEN, 1), lambda s: (s, 0, 0)),
        pl.BlockSpec((1, 1, LEN), lambda s: (s, 0, 0)),
    ]


def attend(projected, labels):
    rows, width = projected.shape[0], projected.shape[1] // 3
    count, heads = rows // LEN, width // HD
    return pl.pallas_call(
        attend_kernel,
        grid=(count,),
        in_specs=sequence_specs(width),
        out_specs=[
            pl.BlockSpec((LEN, width), lambda s: (s, 0)),
            pl.BlockSpec((1, LEN, heads), lambda s: (s, 0, 0)),
        ],
        out_shape=[
            jax.ShapeDtypeStruct((rows, width), BF),
            jax.ShapeDtypeStruct((count, LEN, heads), F32),
        ],
        cost_estimate=pl.CostEstimate(
            flops=count * 4 * LEN * LEN * width * heads,
            bytes_accessed=rows * width * 8,
            transcendentals=count * heads * LEN * LEN,
        ),
        name="attend",
    )(projected, projected, projected, labels[:, :, None], labels[:, None, :])


def attend_back(projected, labels, dcontext, log_total):
    rows, width = projected.shape[0], projected.shape[1] // 3
    count, heads = rows // LEN, width // HD
    return pl.pallas_call(
        attend_back_kernel,
        grid=(count,),
        in_specs=sequence_specs(width)
        + [
            pl.BlockSpec((LEN, width), lambda s: (s, 0)),
            pl.BlockSpec((1, LEN, heads), lambda s: (s, 0, 0)),
        ],
        out_specs=pl.BlockSpec((LEN, 3 * width), lambda s: (s, 0)),
        out_shape=jax.ShapeDtypeStruct((rows, 3 * width), BF),
        cost_estimate=pl.CostEstimate(
            flops=count * 10 * LEN * LEN * width * heads,
            bytes_accessed=rows * width * 14,
            transcendentals=count * heads * LEN * LEN,
        ),
        name="attend_back",
    )(
        projected,
        projected,
        projected,
        labels[:, :, None],
        labels[:, None, :],
        dcontext,
        log_total,
    )


def norm(values):
    center = values - jnp.mean(values, axis=1, keepdims=True)
    inverse = lax.rsqrt(jnp.mean(center * center, axis=1, keepdims=True) + EPSILON)
    return center * inverse, inverse


def norm_back(scaled, normed, inverse):
    mean = jnp.mean(scaled, axis=1, keepdims=True)
    along = jnp.mean(scaled * normed, axis=1, keepdims=True)
    return inverse * (scaled - mean - normed * along)


def gelu_both(pre_act):
    cdf = 0.5 * (1.0 + lax.erf(pre_act * (2.0**-0.5)))
    slope = cdf + pre_act * jnp.exp(-0.5 * pre_act * pre_act) * ((2.0 * math.pi) ** -0.5)
    return (pre_act * cdf).astype(BF), slope.astype(BF)


def total_of(parts):
    return functools.reduce(lambda a, b: a + b, parts)


def local(
    tokens,
    segment_ids,
    w_query,
    w_key,
    w_value,
    b_query,
    b_value,
    w_out,
    b_out,
    gain_one,
    bias_one,
    w_in,
    b_in,
    w_down,
    b_down,
    gain_two,
    bias_two,
    cotangent,
):
    t = lax.axis_index("tensor")
    d = lax.axis_index("dp")
    ways = 4
    row_count = tokens.shape[0]
    width = w_query.shape[0]
    cols = w_query.shape[1]
    sequences = row_count // LEN
    chunks = CHUNKS if sum(CHUNKS) == sequences else (sequences,)
    labels = segment_ids.reshape(sequences, LEN)

    def blocks_of(values, axis=0):
        return jnp.split(values, ways, axis=axis)

    def rows_rel(values):
        r = values.shape[0] // ways
        return [lax.dynamic_slice_in_dim(values, (t ^ k) * r, r, 0) for k in range(ways)]

    vectors = jnp.stack([b_out, gain_one, bias_one, b_down, gain_two, bias_two])
    vectors = jnp.concatenate(xor_order(gather_blocks(vectors), t), axis=1).astype(F32)
    b_out_f, gain_one_f, bias_one_f, b_down_f, gain_two_f, bias_two_f = (
        vectors[i : i + 1] for i in range(6)
    )
    proj_weight = jnp.concatenate([w_query, w_key, w_value], axis=1)
    proj_bias = jnp.concatenate([b_query.astype(F32), jnp.zeros((cols,), F32), b_value.astype(F32)])
    weight_rel = jnp.concatenate(rows_rel(proj_weight), axis=0)

    first = 0
    spans = []
    for count in chunks:
        spans.append((first, count))
        first += count

    xs, projs, ctxs, totals, z_ones = [], [], [], [], []
    for start, count in spans:
        mine = tokens[start * LEN : (start + count) * LEN]
        xs.append(jnp.concatenate(xor_order(gather_blocks(mine), t), axis=1))
    cots = []
    for start, count in spans:
        mine = cotangent[start * LEN : (start + count) * LEN]
        cots.append(jnp.concatenate(xor_order(exchange_blocks(rows_rel(mine)), t), axis=1))

    h_ones, n_ones, inv_ones, h_rels = [], [], [], []
    for i, (start, count) in enumerate(spans):
        proj = (mm(xs[i], proj_weight) + proj_bias).astype(BF)
        context, log_total = attend(proj, labels[start : start + count])
        ctx_rel = jnp.concatenate(rows_rel(context), axis=0)
        part = mm(ctx_rel, w_out).astype(BF)
        attn = scatter_sum(blocks_of(part))
        r = count * LEN // ways
        x_mine = lax.dynamic_slice_in_dim(xs[i], t * r, r, 0)
        z_one = x_mine.astype(F32) + attn + b_out_f
        n_one, inv_one = norm(z_one)
        h_one = n_one * gain_one_f + bias_one_f
        projs.append(proj)
        ctxs.append(ctx_rel)
        totals.append(log_total)
        h_ones.append(h_one)
        n_ones.append(n_one)
        inv_ones.append(inv_one)
        h_rels.append(jnp.concatenate(gather_blocks(h_one.astype(BF)), axis=0))

    outs, dz_twos, dz_rels, hiddens, slopes = [], [], [], [], []
    gain_two_parts, bias_two_parts, b_down_parts = [], [], []
    for i, (start, count) in enumerate(spans):
        pre_act = mm(h_rels[i], w_in) + b_in.astype(F32)
        hidden, slope = gelu_both(pre_act)
        part = mm(hidden, w_down).astype(BF)
        z_two = h_ones[i] + scatter_sum(blocks_of(part)) + b_down_f
        n_two, inv_two = norm(z_two)
        result = (n_two * gain_two_f + bias_two_f).astype(BF)
        grad_out = cots[i].astype(F32)
        gain_two_parts.append(jnp.sum(grad_out * n_two, axis=0))
        bias_two_parts.append(jnp.sum(grad_out, axis=0))
        dz_two = norm_back(grad_out * gain_two_f, n_two, inv_two)
        b_down_parts.append(jnp.sum(dz_two, axis=0))
        dz_twos.append(dz_two)
        hiddens.append(hidden)
        slopes.append(slope)
        dz_rels.append(jnp.concatenate(gather_blocks(dz_two.astype(BF)), axis=0))
        rel_cols = [
            lax.dynamic_slice_in_dim(result, (t ^ k) * cols, cols, 1) for k in range(ways)
        ]
        outs.append(jnp.concatenate(xor_order(exchange_blocks(rel_cols), t), axis=0))

    dz_ones, dz1_rels, dpres = [], [], []
    gain_one_parts, bias_one_parts, b_out_parts, b_in_parts = [], [], [], []
    for i, (start, count) in enumerate(spans):
        dhidden = against(dz_rels[i], w_down)
        dpre = (dhidden * slopes[i].astype(F32)).astype(BF)
        b_in_parts.append(jnp.sum(dpre.astype(F32), axis=0))
        part = against(dpre, w_in).astype(BF)
        dh_one = dz_twos[i] + scatter_sum(blocks_of(part))
        gain_one_parts.append(jnp.sum(dh_one * n_ones[i], axis=0))
        bias_one_parts.append(jnp.sum(dh_one, axis=0))
        dz_one = norm_back(dh_one * gain_one_f, n_ones[i], inv_ones[i])
        b_out_parts.append(jnp.sum(dz_one, axis=0))
        dpres.append(dpre)
        dz1_rels.append(jnp.concatenate(gather_blocks(dz_one.astype(BF)), axis=0))

    def all_rows(parts):
        return parts[0] if len(parts) == 1 else jnp.concatenate(parts, axis=0)

    grad_w_down = summed_big(over_rows(all_rows(hiddens), all_rows(dz_rels)), 0, d)
    grad_w_in = summed_big(over_rows(all_rows(h_rels), all_rows(dpres)), 1, d)

    grad_tokens, dprojs = [], []
    for i, (start, count) in enumerate(spans):
        dcontext = against(dz1_rels[i], w_out).astype(BF)
        dcontext = jnp.concatenate(rows_rel(dcontext), axis=0)
        dproj = attend_back(projs[i], labels[start : start + count], dcontext, totals[i])
        dprojs.append(dproj)
        part = against(dproj, weight_rel).astype(BF)
        dz_cols = lax.dynamic_slice_in_dim(dz1_rels[i], t * cols, cols, 1)
        dz_cols = jnp.concatenate(rows_rel(dz_cols), axis=0)
        summed = scatter_sum(blocks_of(part, axis=1))
        grad_tokens.append((dz_cols.astype(F32) + summed).astype(BF))

    grad_w_out = summed_big(over_rows(all_rows(ctxs), all_rows(dz1_rels)), 0, d)
    dproj_all = all_rows(dprojs)
    grad_proj = summed_big(over_rows(all_rows(xs), dproj_all), 1, d)
    b_proj = jnp.sum(dproj_all.astype(F32), axis=0).reshape(3, cols)

    wide = jnp.stack(
        [
            total_of(p)
            for p in (
                gain_two_parts,
                bias_two_parts,
                b_down_parts,
                gain_one_parts,
                bias_one_parts,
                b_out_parts,
            )
        ]
    )
    wide_rel = [lax.dynamic_slice_in_dim(wide, (t ^ k) * cols, cols, 1) for k in range(ways)]
    narrow = total_of(exchange_blocks(wide_rel))
    b_in_sum = total_of(b_in_parts).reshape(-1, cols)
    small = summed_small(jnp.concatenate([narrow, b_in_sum], axis=0))
    b_proj = summed_small(b_proj)

    return (
        all_rows(outs),
        all_rows(grad_tokens),
        grad_proj[:, :cols],
        grad_proj[:, cols : 2 * cols],
        grad_proj[:, 2 * cols :],
        b_proj[0],
        b_proj[2],
        grad_w_out,
        small[5],
        small[3],
        small[4],
        grad_w_in,
        small[6:].reshape(-1),
        grad_w_down,
        small[2],
        small[0],
        small[1],
    )


def solution(mesh):
    placed = (
        P("dp", "tensor"),
        P("dp"),
        P(None, "tensor"),
        P(None, "tensor"),
        P(None, "tensor"),
        P("tensor"),
        P("tensor"),
        P("tensor", None),
        P("tensor"),
        P("tensor"),
        P("tensor"),
        P(None, "tensor"),
        P("tensor"),
        P("tensor", None),
        P("tensor"),
        P("tensor"),
        P("tensor"),
        P("dp", "tensor"),
    )
    return jax.shard_map(
        local,
        mesh=mesh,
        in_specs=placed,
        out_specs=(
            P("dp", "tensor"),
            P("dp", "tensor"),
            P(None, "tensor"),
            P(None, "tensor"),
            P(None, "tensor"),
            P("tensor"),
            P("tensor"),
            P("tensor", None),
            P("tensor"),
            P("tensor"),
            P("tensor"),
            P(None, "tensor"),
            P("tensor"),
            P("tensor", None),
            P("tensor"),
            P("tensor"),
            P("tensor"),
        ),
        check_vma=False,
    )
```

```python
import functools
import math

import jax
import jax.numpy as jnp
from jax import lax
from jax.experimental import pallas as pl
from jax.experimental.pallas import tpu as pltpu
from jax.sharding import PartitionSpec as P

HD = 64
LEN = 512

EPSILON = 1e-05
MASKED = -1000000000.0
VMEM_LIMIT = 16 << 20
BF = jnp.bfloat16
F32 = jnp.float32


def mm(left, right):
    return lax.dot_general(left, right, (((1,), (0,)), ((), ())), preferred_element_type=F32)


def over_rows(left, right):
    return lax.dot_general(left, right, (((0,), (0,)), ((), ())), preferred_element_type=F32)


def against(left, right):
    return lax.dot_general(left, right, (((1,), (1,)), ((), ())), preferred_element_type=F32)


def swap(values, axis, bit):
    size = lax.axis_size(axis)
    return lax.ppermute(values, axis, [(i, i ^ bit) for i in range(size)])


def gather_blocks(own):
    across = swap(own, "tensor", 2)
    beside = swap(own, "tensor", 1)
    corner = swap(across, "tensor", 1)
    return own, beside, across, corner


def exchange_blocks(blocks):
    return (
        blocks[0],
        swap(blocks[1], "tensor", 1),
        swap(blocks[2], "tensor", 2),
        swap(blocks[3], "tensor", 3),
    )


def scatter_terms(b0, b1, b2, b3):
    far = swap(b3, "tensor", 1)
    near = swap(b1, "tensor", 1)
    onward = (b2.astype(F32) + far.astype(F32)).astype(BF)
    return b0, near, swap(onward, "tensor", 2)


def dp_bits(order):
    size = lax.axis_size("dp")
    bits = [1 << i for i in range(int(math.log2(size)))]
    if order and len(bits) > 1:
        bits[0], bits[1] = bits[1], bits[0]
    return bits


def summed_small(values):
    for bit in dp_bits(0):
        values = values + swap(values, "dp", bit)
    return values


class Line:
    def __init__(self, place):
        self.place = place

    def __call__(self, kernel, name, out_shape, operands, flops=0, exps=0, scratch=()):
        out_shape = [jax.ShapeDtypeStruct(s, d) for s, d in out_shape]
        size = sum(math.prod(o.shape) * o.dtype.itemsize for o in list(operands) + out_shape)
        whole = pl.BlockSpec(memory_space=pltpu.VMEM)
        outs = pl.pallas_call(
            kernel,
            in_specs=[pl.BlockSpec(memory_space=pltpu.SMEM)] + [whole] * len(operands),
            out_specs=[whole] * len(out_shape),
            out_shape=out_shape,
            scratch_shapes=list(scratch),
            compiler_params=pltpu.CompilerParams(vmem_limit_bytes=VMEM_LIMIT),
            cost_estimate=pl.CostEstimate(flops=flops, transcendentals=exps, bytes_accessed=size),
            name=name,
        )(self.place, *operands)
        last = min(outs, key=lambda o: math.prod(o.shape))
        self.place, _ = lax.optimization_barrier((self.place, last))
        return outs


def block(index, size):
    return pl.ds(pl.multiple_of(index * size, size), size)


def head_lanes(width, head):
    lane = lax.broadcasted_iota(jnp.int32, (1, width), 1)
    return (lane >= head * HD) & (lane < (head + 1) * HD)


def allowed_block(label_row):
    length = label_row.shape[1]
    label_row = label_row.astype(F32)
    label_column = jnp.transpose(jnp.broadcast_to(label_row, (8, length)))[:, :1]
    same = label_column == label_row
    diagonal = lax.broadcasted_iota(jnp.int32, (length, length), 0) == lax.broadcasted_iota(
        jnp.int32, (length, length), 1
    )
    return same & ((label_column != 0.0) | diagonal)


def attend_kernel(
    place, p0, p1, p2, p3, wq, wk, wv, bq, bv, label, w_out, proj, ctx, total, residual, keep, send
):
    t = place[0]
    width = wq.shape[1]
    pieces = (p0, p1, p2, p3)
    rows = p0.shape[0] // 4
    for k, piece in enumerate(pieces):
        residual[:, block(t ^ k, width)] = piece[block(t, rows), :]
    parts = []
    for weight in (wq, wk, wv):
        parts.append(total_of([mm(piece[...], weight[block(t ^ k, width), :]) for k, piece in enumerate(pieces)]))
    queries = (parts[0] + bq[...].astype(F32)).astype(BF)
    keys = parts[1].astype(BF)
    values = (parts[2] + bv[...].astype(F32)).astype(BF)
    proj[:, :width] = queries
    proj[:, width : 2 * width] = keys
    proj[:, 2 * width :] = values
    allowed = allowed_block(label[...])
    context = jnp.zeros(queries.shape, F32)
    zero = jnp.zeros((), BF)
    for head in range(width // HD):
        lanes = head_lanes(width, head)
        scores = against(jnp.where(lanes, queries, zero), keys) * (HD**-0.5)
        scores = jnp.where(allowed, scores, MASKED)
        peak = jnp.max(scores, axis=1, keepdims=True)
        terms = jnp.exp(scores - peak)
        summed = jnp.sum(terms, axis=1, keepdims=True)
        probs = (terms / summed).astype(BF)
        context = context + mm(probs, jnp.where(lanes, values, zero))
        total[:, head : head + 1] = peak + jnp.log(summed)
    context = context.astype(BF)
    for j in range(4):
        ctx[block(t ^ j, rows), :] = context[j * rows : (j + 1) * rows]
    for k in range(4):
        part = mm(ctx[k * rows : (k + 1) * rows, :], w_out[...]).astype(BF)
        (send if k % 2 else keep)[k // 2] = part


def attend_back_kernel(
    place, d0, d1, d2, d3, w_out, proj, total, label, wq, wk, wv, dproj, keep, send, dz_cols, bias, dctx
):
    t = place[0]
    width = wq.shape[1]
    rows = d0.shape[0]
    for k, piece in enumerate((d0, d1, d2, d3)):
        dctx[block(t ^ k, rows), :] = against(piece[...], w_out[...]).astype(BF)
        dz_cols[block(t ^ k, rows), :] = piece[:, block(t, width)]
    allowed = allowed_block(label[...])
    queries, keys, values = proj[:, :width], proj[:, width : 2 * width], proj[:, 2 * width :]
    dcontext = dctx[...]
    scale = HD**-0.5
    dquery = jnp.zeros(queries.shape, F32)
    dkey = jnp.zeros(queries.shape, F32)
    dvalue = jnp.zeros(queries.shape, F32)
    zero = jnp.zeros((), BF)
    for head in range(width // HD):
        lanes = head_lanes(width, head)
        q_head = jnp.where(lanes, queries, zero)
        d_head = jnp.where(lanes, dcontext, zero)
        k_head = jnp.where(lanes, keys, zero)
        scores = against(q_head, keys) * scale
        scores = jnp.where(allowed, scores, MASKED)
        probs = jnp.exp(scores - total[:, head : head + 1])
        dprobs = against(d_head, values)
        delta = jnp.sum(probs * dprobs, axis=1, keepdims=True)
        dscores = (probs * (dprobs - delta)).astype(BF)
        dquery = dquery + mm(dscores, k_head)
        dkey = dkey + over_rows(dscores, q_head)
        dvalue = dvalue + over_rows(probs.astype(BF), d_head)
    grads = ((dquery * scale).astype(BF), (dkey * scale).astype(BF), dvalue.astype(BF))
    for i, grad in enumerate(grads):
        dproj[:, i * width : (i + 1) * width] = grad
        bias[:, i * width : (i + 1) * width] = jnp.sum(grad.astype(F32), axis=0, keepdims=True)
    for k in range(4):
        here = block(t ^ k, width)
        part = total_of([against(grad, weight[here, :]) for grad, weight in zip(grads, (wq, wk, wv))])
        (send if k % 2 else keep)[k // 2] = part.astype(BF)


def normed_of(values):
    center = values - jnp.mean(values, axis=1, keepdims=True)
    inverse = lax.rsqrt(jnp.mean(center * center, axis=1, keepdims=True) + EPSILON)
    return center * inverse, inverse


def norm_back(scaled, normed, inverse):
    mean = jnp.mean(scaled, axis=1, keepdims=True)
    along = jnp.mean(scaled * normed, axis=1, keepdims=True)
    return inverse * (scaled - mean - normed * along)


def fill(vectors, spread, t):
    width = vectors[0].shape[1]
    for k, ref in enumerate(vectors):
        spread[0:6, block(t ^ k, width)] = ref[...].astype(F32)


def first_norm_kernel(place, s0, s1, s2, residual, v0, v1, v2, v3, normed_ref, inverse_ref, low, spread):
    fill((v0, v1, v2, v3), spread, place[0])
    z = s0[...].astype(F32) + s1[...].astype(F32) + s2[...].astype(F32)
    z = residual[...].astype(F32) + z + spread[0:1, :]
    normed, inverse = normed_of(z)
    normed_ref[...] = normed
    inverse_ref[...] = inverse
    low[...] = (normed * spread[1:2, :] + spread[2:3, :]).astype(BF)


def second_norm_kernel(
    place, s0, s1, s2, normed_one, c0, c1, c2, c3, v0, v1, v2, v3, dz, low, out, sums, spread, cots
):
    t = place[0]
    fill((v0, v1, v2, v3), spread, t)
    width = c0.shape[1]
    for k, ref in enumerate((c0, c1, c2, c3)):
        cots[:, block(t ^ k, width)] = ref[...].astype(F32)
    h_one = normed_one[...] * spread[1:2, :] + spread[2:3, :]
    z = h_one + (s0[...].astype(F32) + s1[...].astype(F32) + s2[...].astype(F32)) + spread[3:4, :]
    normed, inverse = normed_of(z)
    out[...] = (normed * spread[4:5, :] + spread[5:6, :]).astype(BF)
    grad = cots[...]
    sums[0:1, :] = jnp.sum(grad * normed, axis=0, keepdims=True)
    sums[1:2, :] = jnp.sum(grad, axis=0, keepdims=True)
    back = norm_back(grad * spread[4:5, :], normed, inverse)
    sums[2:3, :] = jnp.sum(back, axis=0, keepdims=True)
    dz[...] = back
    low[...] = back.astype(BF)


def first_back_kernel(place, s0, s1, s2, dz, normed_ref, inverse_ref, v0, v1, v2, v3, low, sums, spread):
    fill((v0, v1, v2, v3), spread, place[0])
    dh = dz[...] + (s0[...].astype(F32) + s1[...].astype(F32) + s2[...].astype(F32))
    normed = normed_ref[...]
    sums[0:1, :] = jnp.sum(dh * normed, axis=0, keepdims=True)
    sums[1:2, :] = jnp.sum(dh, axis=0, keepdims=True)
    back = norm_back(dh * spread[1:2, :], normed, inverse_ref[...])
    sums[2:3, :] = jnp.sum(back, axis=0, keepdims=True)
    low[...] = back.astype(BF)


def feed_kernel(place, h0, h1, w_in, b_in, w_down, hidden, slope, keep, send):
    rows = jnp.concatenate([h0[...], h1[...]], axis=0)
    r = h0.shape[0]
    units = w_in.shape[1]
    step = min(256, units)
    total = jnp.zeros((2 * r, w_down.shape[1]), F32)
    for first in range(0, units, step):
        here = slice(first, first + step)
        pre_act = mm(rows, w_in[:, here]) + b_in[:, here].astype(F32)
        cdf = 0.5 * (1.0 + lax.erf(pre_act * (2.0**-0.5)))
        rise = pre_act * jnp.exp(-0.5 * pre_act * pre_act) * ((2.0 * math.pi) ** -0.5)
        active = (pre_act * cdf).astype(BF)
        hidden[:, here] = active
        slope[:, here] = (cdf + rise).astype(BF)
        total = total + mm(active, w_down[here, :])
    keep[...] = total[:r].astype(BF)
    send[...] = total[r:].astype(BF)


def feed_back_kernel(place, d0, d1, slope, w_down, w_in, dpre, keep, send, bias):
    rows = jnp.concatenate([d0[...], d1[...]], axis=0)
    r = d0.shape[0]
    units = w_in.shape[1]
    step = min(256, units)
    total = jnp.zeros((2 * r, w_in.shape[0]), F32)
    for first in range(0, units, step):
        here = slice(first, first + step)
        grad = (against(rows, w_down[here, :]) * slope[:, here].astype(F32)).astype(BF)
        dpre[:, here] = grad
        bias[:, here] = jnp.sum(grad.astype(F32), axis=0, keepdims=True)
        total = total + against(grad, w_in[:, here])
    keep[...] = total[:r].astype(BF)
    send[...] = total[r:].astype(BF)


def weight_grad_kernel(groups, stacked, bit, place, *refs):
    keep, send = refs[-2:]
    set_bit = jnp.where((place[1] & bit) == 0, 0, 1)
    lefts, rights = [], []
    at = 0
    for left, right in groups:
        lefts.append(refs[at : at + left])
        rights.append(refs[at + left : at + left + right])
        at += left + right

    def joined(parts, columns):
        parts = [p[:, columns] for p in parts]
        return parts[0] if len(parts) == 1 else jnp.concatenate(parts, axis=0)

    half, width = keep.shape
    step = min(256, half)
    for half_index, out in ((1 - set_bit, send), (set_bit, keep)):
        for first in range(0, half, step):
            here = block(half_index * (half // step) + first // step, step)
            if stacked:
                terms = [over_rows(joined(l, slice(None)), joined(r, here)) for l, r in zip(lefts, rights)]
            else:
                terms = [over_rows(joined(l, here), joined(r, slice(None))) for l, r in zip(lefts, rights)]
            out[first : first + step, :] = total_of(terms).astype(BF)


def weight_grad(line, pairs, height, width, bit, name, stacked=False):
    operands = [x for left, right in pairs for x in (*left, *right)]
    groups = [(len(left), len(right)) for left, right in pairs]
    depth = sum(x.shape[0] for left, _ in pairs for x in left)
    return line(
        functools.partial(weight_grad_kernel, groups, stacked, bit),
        name,
        [((height // 2, width), BF)] * 2,
        operands,
        flops=2 * depth * height * width,
    )


def proj_grad_kernel(count, bits, place, *refs):
    t = place[0]
    outs, full = refs[-7:-1], refs[-1]
    size = refs[0].shape[1]
    for k in range(4):
        full[block(t ^ k, size), :] = total_of(
            [over_rows(refs[4 * i + k][...], refs[4 * count + i][...]) for i in range(count)]
        ).astype(BF)
    half = outs[0].shape[0]
    for j, bit in enumerate(bits):
        set_bit = jnp.where((place[1] & bit) == 0, 0, 1)
        columns = slice(j * size, (j + 1) * size)
        outs[2 * j][...] = full[block(set_bit, half), columns]
        outs[2 * j + 1][...] = full[block(1 - set_bit, half), columns]


def halve_kernel(bit, place, kept, got, keep, send):
    set_bit = jnp.where((place[1] & bit) == 0, 0, 1)
    half = keep.shape[0]
    for index, out in ((1 - set_bit, send), (set_bit, keep)):
        here = block(index, half)
        out[...] = (kept[here, :].astype(F32) + got[here, :].astype(F32)).astype(BF)


def add_kernel(place, kept, got, out):
    out[...] = (kept[...].astype(F32) + got[...].astype(F32)).astype(BF)


def join_kernel(bit, unstack, place, mine, got, out):
    set_bit = jnp.where((place[1] & bit) == 0, 0, 1)
    half = mine.shape[0]
    for index, ref in ((set_bit, mine), (1 - set_bit, got)):
        if unstack:
            tall = out.shape[0]
            for j in range(half // tall):
                columns = block(index * (half // tall) + j, ref.shape[1])
                out[:, columns] = ref[j * tall : (j + 1) * tall, :].astype(out.dtype)
        else:
            out[block(index, half), :] = ref[...].astype(out.dtype)


def dp_sum(line, keep, send, bits, name, unstack=None):
    got = swap(send, "dp", bits[0])
    yield
    half, width = keep.shape
    for bit in bits[1:]:
        half //= 2
        keep, send = line(
            functools.partial(halve_kernel, bit), name + "_halve", [((half, width), BF)] * 2, [keep, got]
        )
        got = swap(send, "dp", bit)
        yield
    (mine,) = line(add_kernel, name + "_add", [((half, width), BF)], [keep, got])
    got = swap(mine, "dp", bits[-1])
    yield
    for bit in reversed(bits[1:]):
        half *= 2
        (mine,) = line(
            functools.partial(join_kernel, bit, False), name + "_join", [((half, width), BF)], [mine, got]
        )
        got = swap(mine, "dp", bits[bits.index(bit) - 1])
        yield
    (result,) = line(
        functools.partial(join_kernel, bits[0], unstack is not None),
        name + "_whole",
        [(unstack or (2 * half, width), F32)],
        [mine, got],
    )
    return result


class Steps:
    def __init__(self, generator):
        self.generator = generator
        self.result = None
        self.go()

    def go(self, times=1):
        for _ in range(times):
            if self.result is None:
                try:
                    next(self.generator)
                except StopIteration as stop:
                    self.result = stop.value

    def finish(self):
        while self.result is None:
            self.go()
        return self.result


def out_pack_kernel(count, place, *refs):
    t = place[0]
    r = refs[0].shape[0]
    for k, out in enumerate(refs[count:]):
        for i in range(count):
            out[i * r : (i + 1) * r, :] = refs[i][:, block(t ^ k, out.shape[1])]


def rows_kernel(count, place, *refs):
    t = place[0]
    out = refs[-1]
    r = refs[0].shape[0] // count
    for k in range(4):
        for i in range(count):
            out[block(4 * i + (t ^ k), r), :] = refs[k][i * r : (i + 1) * r, :]


def tokens_kernel(place, *refs):
    out = refs[-1]
    r = refs[0].shape[0]
    for i in range((len(refs) - 1) // 4):
        terms = [refs[4 * i + j][...].astype(F32) for j in range(4)]
        out[i * r : (i + 1) * r, :] = total_of(terms).astype(BF)


def pack_kernel(count, place, *refs):
    t = place[0]
    outs, spread = refs[2 * count : 2 * count + 4], refs[-1]
    spread[0:3, :] = total_of([refs[i][...] for i in range(count)])
    spread[3:6, :] = total_of([refs[count + i][...] for i in range(count)])
    width = outs[0].shape[1]
    for k, ref in enumerate(outs):
        ref[...] = spread[0:6, block(t ^ k, width)]


def total_of(parts):
    return functools.reduce(lambda a, b: a + b, parts)


def local(
    tokens,
    segment_ids,
    w_query,
    w_key,
    w_value,
    b_query,
    b_value,
    w_out,
    b_out,
    gain_one,
    bias_one,
    w_in,
    b_in,
    w_down,
    b_down,
    gain_two,
    bias_two,
    cotangent,
):
    t = lax.axis_index("tensor")
    d = lax.axis_index("dp")
    line = Line(jnp.stack([t, d]).astype(jnp.int32))
    row_count, cols = tokens.shape
    width = w_query.shape[0]
    units = w_in.shape[1]
    count = row_count // LEN
    r = LEN // 4
    heads = cols // HD
    labels = segment_ids.reshape(count, 1, LEN)
    every = range(count)
    spread = pltpu.VMEM((8, width), F32)

    pieces = [gather_blocks(tokens[i * LEN : (i + 1) * LEN]) for i in every]
    vectors = jnp.stack([b_out, gain_one, bias_one, b_down, gain_two, bias_two])
    vectors, cotangent, _ = lax.optimization_barrier((vectors, cotangent, pieces[-1][2]))
    vectors = gather_blocks(vectors)
    by_rows = cotangent.reshape(count, 4, r, cols)
    cots = exchange_blocks(
        [lax.dynamic_slice_in_dim(by_rows, t ^ k, 1, 1).reshape(count * r, cols) for k in range(4)]
    )

    ctxs, projs, totals, attn_terms = [], [], [], []

    def do_attend(i):
        proj, ctx, total, residual, keep, send = line(
            attend_kernel,
            "attend",
            [
                ((LEN, 3 * cols), BF),
                ((LEN, cols), BF),
                ((LEN, heads), F32),
                ((r, width), BF),
                ((2, r, width), BF),
                ((2, r, width), BF),
            ],
            [*pieces[i], w_query, w_key, w_value, b_query[None], b_value[None], labels[i], w_out],
            flops=2 * LEN * width * 4 * cols + 4 * LEN * LEN * cols * heads,
            exps=heads * LEN * LEN,
        )
        sent = swap(send, "tensor", 1)
        onward = (keep[1].astype(F32) + sent[1].astype(F32)).astype(BF)
        attn_terms.append([keep[0], sent[0], swap(onward, "tensor", 2), residual])
        projs.append(proj)
        ctxs.append(ctx)
        totals.append(total)

    firsts, h_pieces = [], []

    def do_first_norm(i):
        normed, inverse, low = line(
            first_norm_kernel,
            "first_norm",
            [((r, width), F32), ((r, 1), F32), ((r, width), BF)],
            [*attn_terms[i], *vectors],
            flops=20 * r * width,
            scratch=[spread],
        )
        firsts.append((normed, inverse))
        h_pieces.append(gather_blocks(low))

    feeds = {}

    def do_feed(i, j):
        feeds[i, j] = line(
            feed_kernel,
            "feed",
            [((2 * r, units), BF), ((2 * r, units), BF), ((r, width), BF), ((r, width), BF)],
            [*h_pieces[i][2 * j : 2 * j + 2], w_in, b_in[None], w_down],
            flops=8 * r * width * units,
            exps=2 * r * units * 2,
        )

    seconds, dz_pieces, results = [], [], []

    def do_second_norm(i):
        dz, low, result, sums = line(
            second_norm_kernel,
            "second_norm",
            [((r, width), F32), ((r, width), BF), ((r, width), BF), ((3, width), F32)],
            [
                *scatter_terms(*feeds[i, 0][2:], *feeds[i, 1][2:]),
                firsts[i][0],
                *[c[i * r : (i + 1) * r] for c in cots],
                *vectors,
            ],
            flops=40 * r * width,
            scratch=[spread, pltpu.VMEM((r, width), F32)],
        )
        seconds.append((dz, sums))
        results.append(result)
        dz_pieces.append(gather_blocks(low))

    backs = {}

    def do_feed_back(i, j):
        backs[i, j] = line(
            feed_back_kernel,
            "feed_back",
            [((2 * r, units), BF), ((r, width), BF), ((r, width), BF), ((1, units), F32)],
            [*dz_pieces[i][2 * j : 2 * j + 2], feeds[i, j][1], w_down, w_in],
            flops=8 * r * width * units,
        )

    thirds, dz1_pieces = [], []

    def do_first_back(i):
        low, sums = line(
            first_back_kernel,
            "first_back",
            [((r, width), BF), ((3, width), F32)],
            [*scatter_terms(*backs[i, 0][1:3], *backs[i, 1][1:3]), seconds[i][0], *firsts[i], *vectors],
            flops=30 * r * width,
            scratch=[spread],
        )
        thirds.append(sums)
        dz1_pieces.append(gather_blocks(low))

    dprojs, token_terms, b_proj_parts = [], [], []

    def do_attend_back(i):
        dproj, keep, send, dz_cols, bias = line(
            attend_back_kernel,
            "attend_back",
            [
                ((LEN, 3 * cols), BF),
                ((2, LEN, cols), BF),
                ((2, LEN, cols), BF),
                ((LEN, cols), BF),
                ((1, 3 * cols), F32),
            ],
            [*dz1_pieces[i], w_out, projs[i], totals[i], labels[i], w_query, w_key, w_value],
            flops=2 * LEN * width * 4 * cols + 10 * LEN * LEN * cols * heads,
            exps=heads * LEN * LEN,
            scratch=[pltpu.VMEM((LEN, cols), BF)],
        )
        sent = swap(send, "tensor", 1)
        onward = (keep[1].astype(F32) + sent[1].astype(F32)).astype(BF)
        token_terms.extend([dz_cols, keep[0], sent[0], swap(onward, "tensor", 2)])
        dprojs.append(dproj)
        b_proj_parts.append(bias)

    for i in every:
        do_attend(i)
    for i in every:
        do_first_norm(i)
        do_feed(i, 0)
    for i in every:
        do_feed(i, 1)
    for i in every:
        do_second_norm(i)
        do_feed_back(i, 0)
    for i in every:
        do_feed_back(i, 1)

    early, late = dp_bits(0), dp_bits(1)
    down_pairs = [
        ([feeds[i, j][0]], dz_pieces[i][2 * j : 2 * j + 2]) for i in every for j in range(2)
    ]
    down = Steps(
        dp_sum(line, *weight_grad(line, down_pairs, units, width, early[0], "down_grad"), early, "down")
    )
    do_first_back(0)
    in_pairs = [
        (h_pieces[i][2 * j : 2 * j + 2], [backs[i, j][0]]) for i in every for j in range(2)
    ]
    into = Steps(
        dp_sum(line, *weight_grad(line, in_pairs, width, units, late[0], "in_grad"), late, "into")
    )
    for i in every[1:]:
        do_first_back(i)
    pieces_out = exchange_blocks(
        line(
            functools.partial(out_pack_kernel, count),
            "out_pack",
            [((count * r, cols), BF)] * 4,
            results,
        )
    )
    wide = line(
        functools.partial(pack_kernel, count),
        "pack",
        [((6, cols), F32)] * 4,
        [s for _, s in seconds] + thirds,
        scratch=[spread],
    )
    narrow = total_of(exchange_blocks(wide))
    b_in_sum = total_of([b[3] for b in backs.values()])
    small = summed_small(jnp.concatenate([narrow, b_in_sum.reshape(-1, cols)], axis=0))

    for i in every:
        do_attend_back(i)
        down.go()
        into.go()
    out_pairs = [([ctxs[i]], [dz1_pieces[i][k] for k in range(4)]) for i in every]
    outer = Steps(
        dp_sum(
            line,
            *weight_grad(line, out_pairs, width, cols, late[0], "out_grad", stacked=True),
            late,
            "outer",
            unstack=(cols, width),
        )
    )
    orders = (early, late, early)
    grads = line(
        functools.partial(proj_grad_kernel, count, [o[0] for o in orders]),
        "proj_grad",
        [((width // 2, cols), BF)] * 6,
        [p for i in every for p in pieces[i]] + dprojs,
        flops=2 * row_count * width * 3 * cols,
        scratch=[pltpu.VMEM((width, 3 * cols), BF)],
    )
    projections = [
        Steps(dp_sum(line, grads[2 * j], grads[2 * j + 1], order, name))
        for j, (order, name) in enumerate(zip(orders, ("query", "key", "value")))
    ]
    b_proj = summed_small(total_of(b_proj_parts))
    (result,) = line(
        functools.partial(rows_kernel, count), "out_rows", [((row_count, cols), BF)], pieces_out
    )
    waiting = [down, into, outer, *projections]
    while any(s.result is None for s in waiting):
        for s in waiting:
            s.go()
    (grad_tokens,) = line(tokens_kernel, "token_rows", [((row_count, cols), BF)], token_terms)

    return (
        result,
        grad_tokens,
        projections[0].result,
        projections[1].result,
        projections[2].result,
        b_proj[0, :cols],
        b_proj[0, 2 * cols :],
        outer.result,
        small[5],
        small[3],
        small[4],
        into.result,
        small[6:].reshape(-1),
        down.result,
        small[2],
        small[0],
        small[1],
    )


def solution(mesh):
    placed = (
        P("dp", "tensor"),
        P("dp"),
        P(None, "tensor"),
        P(None, "tensor"),
        P(None, "tensor"),
        P("tensor"),
        P("tensor"),
        P("tensor", None),
        P("tensor"),
        P("tensor"),
        P("tensor"),
        P(None, "tensor"),
        P("tensor"),
        P("tensor", None),
        P("tensor"),
        P("tensor"),
        P("tensor"),
        P("dp", "tensor"),
    )
    return jax.shard_map(
        local,
        mesh=mesh,
        in_specs=placed,
        out_specs=(
            P("dp", "tensor"),
            P("dp", "tensor"),
            P(None, "tensor"),
            P(None, "tensor"),
            P(None, "tensor"),
            P("tensor"),
            P("tensor"),
            P("tensor", None),
            P("tensor"),
            P("tensor"),
            P("tensor"),
            P(None, "tensor"),
            P("tensor"),
            P("tensor", None),
            P("tensor"),
            P("tensor"),
            P("tensor"),
        ),
        check_vma=False,
    )
```

```python
import functools
import math

import jax
import jax.numpy as jnp
from jax import lax
from jax.experimental import pallas as pl
from jax.experimental.pallas import tpu as pltpu
from jax.sharding import PartitionSpec as P

HD = 64
LEN = 512

EPSILON = 1e-05
MASKED = -1000000000.0
VMEM_LIMIT = 8 << 20
BF = jnp.bfloat16
F32 = jnp.float32


def mm(left, right):
    return lax.dot_general(left, right, (((1,), (0,)), ((), ())), preferred_element_type=F32)


def over_rows(left, right):
    return lax.dot_general(left, right, (((0,), (0,)), ((), ())), preferred_element_type=F32)


def against(left, right):
    return lax.dot_general(left, right, (((1,), (1,)), ((), ())), preferred_element_type=F32)


def swap(values, axis, bit):
    size = lax.axis_size(axis)
    return lax.ppermute(values, axis, [(i, i ^ bit) for i in range(size)])


def gather_blocks(own):
    across = swap(own, "tensor", 2)
    beside = swap(own, "tensor", 1)
    corner = swap(across, "tensor", 1)
    return own, beside, across, corner


def exchange_blocks(blocks):
    return (
        blocks[0],
        swap(blocks[1], "tensor", 1),
        swap(blocks[2], "tensor", 2),
        swap(blocks[3], "tensor", 3),
    )


def dp_bits(order):
    size = lax.axis_size("dp")
    bits = [1 << i for i in range(int(math.log2(size)))]
    if order and len(bits) > 1:
        bits[0], bits[1] = bits[1], bits[0]
    return bits


class Line:
    def __init__(self, place):
        self.place = place

    def __call__(self, kernel, name, out_shape, operands, flops=0, exps=0, scratch=()):
        out_shape = [jax.ShapeDtypeStruct(s, d) for s, d in out_shape]
        size = sum(math.prod(o.shape) * o.dtype.itemsize for o in list(operands) + out_shape)
        whole = pl.BlockSpec(memory_space=pltpu.VMEM)
        outs = pl.pallas_call(
            kernel,
            in_specs=[pl.BlockSpec(memory_space=pltpu.SMEM)] + [whole] * len(operands),
            out_specs=[whole] * len(out_shape),
            out_shape=out_shape,
            scratch_shapes=list(scratch),
            compiler_params=pltpu.CompilerParams(vmem_limit_bytes=VMEM_LIMIT),
            cost_estimate=pl.CostEstimate(flops=flops, transcendentals=exps, bytes_accessed=size),
            name=name,
        )(self.place, *operands)
        last = min(outs, key=lambda o: math.prod(o.shape))
        self.place, _ = lax.optimization_barrier((self.place, last))
        return outs

    def after(self, value):
        return lax.optimization_barrier((value, self.place))[0]

    def take(self, *values):
        self.place = lax.optimization_barrier((self.place, *values))[0]


def block(index, size):
    return pl.ds(pl.multiple_of(index * size, size), size)


def first_of(ref):
    return (ref[0] if len(ref.shape) == 3 else ref[...]).astype(F32)


def head_lanes(width, head):
    lane = lax.broadcasted_iota(jnp.int32, (1, width), 1)
    return (lane >= head * HD) & (lane < (head + 1) * HD)


def allowed_block(label_row):
    length = label_row.shape[1]
    label_row = label_row.astype(F32)
    label_column = jnp.transpose(jnp.broadcast_to(label_row, (8, length)))[:, :1]
    same = label_column == label_row
    diagonal = lax.broadcasted_iota(jnp.int32, (length, length), 0) == lax.broadcasted_iota(
        jnp.int32, (length, length), 1
    )
    return same & ((label_column != 0.0) | diagonal)


def attend_kernel(
    sequence, place, p0, p1, p2, p3, wq, wk, wv, bq, bv, label, w_out, proj, ctx, total, residual, keep, send
):
    t = place[0]
    width = wq.shape[1]
    length = ctx.shape[0]
    rows = length // 4
    pieces = [p.at[sequence * length : (sequence + 1) * length, :] for p in (p0, p1, p2, p3)]
    for k, piece in enumerate(pieces):
        residual[:, block(t ^ k, width)] = piece[block(t, rows), :]
    parts = []
    for weight in (wq, wk, wv):
        parts.append(total_of([mm(piece[...], weight[block(t ^ k, width), :]) for k, piece in enumerate(pieces)]))
    queries = (parts[0] + bq[...].astype(F32)[None, :]).astype(BF)
    keys = parts[1].astype(BF)
    values = (parts[2] + bv[...].astype(F32)[None, :]).astype(BF)
    proj[:, :width] = queries
    proj[:, width : 2 * width] = keys
    proj[:, 2 * width :] = values
    allowed = allowed_block(label[...])
    context = jnp.zeros(queries.shape, F32)
    zero = jnp.zeros((), BF)
    for head in range(width // HD):
        lanes = head_lanes(width, head)
        scores = against(jnp.where(lanes, queries, zero), keys) * (HD**-0.5)
        scores = jnp.where(allowed, scores, MASKED)
        peak = jnp.max(scores, axis=1, keepdims=True)
        terms = jnp.exp(scores - peak)
        summed = jnp.sum(terms, axis=1, keepdims=True)
        probs = (terms / summed).astype(BF)
        context = context + mm(probs, jnp.where(lanes, values, zero))
        total[:, head : head + 1] = peak + jnp.log(summed)
    context = context.astype(BF)
    for j in range(4):
        ctx[block(t ^ j, rows), :] = context[j * rows : (j + 1) * rows]
    for k in range(4):
        part = mm(ctx[k * rows : (k + 1) * rows, :], w_out[...]).astype(BF)
        (send if k % 2 else keep)[k // 2] = part


def attend_back_kernel(
    place, d0, d1, d2, d3, w_out, proj, total, label, wq, wk, wv, dproj, keep, send, dz_cols, bias, dctx
):
    t = place[0]
    width = wq.shape[1]
    rows = d0.shape[0]
    for k, piece in enumerate((d0, d1, d2, d3)):
        dctx[block(t ^ k, rows), :] = against(piece[...], w_out[...]).astype(BF)
        dz_cols[block(t ^ k, rows), :] = piece[:, block(t, width)]
    allowed = allowed_block(label[...])
    queries, keys, values = proj[:, :width], proj[:, width : 2 * width], proj[:, 2 * width :]
    dcontext = dctx[...]
    scale = HD**-0.5
    dquery = jnp.zeros(queries.shape, F32)
    dkey = jnp.zeros(queries.shape, F32)
    dvalue = jnp.zeros(queries.shape, F32)
    zero = jnp.zeros((), BF)
    for head in range(width // HD):
        lanes = head_lanes(width, head)
        q_head = jnp.where(lanes, queries, zero)
        d_head = jnp.where(lanes, dcontext, zero)
        k_head = jnp.where(lanes, keys, zero)
        scores = against(q_head, keys) * scale
        scores = jnp.where(allowed, scores, MASKED)
        probs = jnp.exp(scores - total[:, head : head + 1])
        dprobs = against(d_head, values)
        delta = jnp.sum(probs * dprobs, axis=1, keepdims=True)
        dscores = (probs * (dprobs - delta)).astype(BF)
        dquery = dquery + mm(dscores, k_head)
        dkey = dkey + over_rows(dscores, q_head)
        dvalue = dvalue + over_rows(probs.astype(BF), d_head)
    grads = ((dquery * scale).astype(BF), (dkey * scale).astype(BF), dvalue.astype(BF))
    for i, grad in enumerate(grads):
        dproj[:, i * width : (i + 1) * width] = grad
        bias[:, i * width : (i + 1) * width] = jnp.sum(grad.astype(F32), axis=0, keepdims=True)
    for k in range(4):
        here = block(t ^ k, width)
        part = total_of([against(grad, weight[here, :]) for grad, weight in zip(grads, (wq, wk, wv))])
        (send if k % 2 else keep)[k // 2] = part.astype(BF)


def normed_of(values):
    center = values - jnp.mean(values, axis=1, keepdims=True)
    inverse = lax.rsqrt(jnp.mean(center * center, axis=1, keepdims=True) + EPSILON)
    return center * inverse, inverse


def norm_back(scaled, normed, inverse):
    mean = jnp.mean(scaled, axis=1, keepdims=True)
    along = jnp.mean(scaled * normed, axis=1, keepdims=True)
    return inverse * (scaled - mean - normed * along)


def fill(vectors, spread, t):
    width = vectors[0].shape[1]
    for k, ref in enumerate(vectors):
        spread[0:6, block(t ^ k, width)] = ref[...].astype(F32)


def onward_kernel(place, kept, got, out):
    out[...] = (kept[...].astype(F32) + got[...].astype(F32)).astype(BF)


def second_of_onward_kernel(place, kept, got, out):
    out[...] = (kept[1].astype(F32) + got[1].astype(F32)).astype(BF)


def vectors_kernel(place, *refs):
    for i, ref in enumerate(refs[:-1]):
        refs[-1][i : i + 1, :] = ref[...][None, :]


def first_norm_kernel(place, s0, s1, s2, residual, v0, v1, v2, v3, normed_ref, inverse_ref, low, spread):
    fill((v0, v1, v2, v3), spread, place[0])
    z = first_of(s0) + first_of(s1) + first_of(s2)
    z = residual[...].astype(F32) + z + spread[0:1, :]
    normed, inverse = normed_of(z)
    normed_ref[...] = normed
    inverse_ref[...] = inverse
    low[...] = (normed * spread[1:2, :] + spread[2:3, :]).astype(BF)


def cot_pack_kernel(count, place, cot, *outs):
    t = place[0]
    r = outs[0].shape[0] // count
    for k, out in enumerate(outs):
        for i in range(count):
            out[i * r : (i + 1) * r, :] = cot[block(4 * i + (t ^ k), r), :]


def second_norm_kernel(
    sequence, place, s0, s1, s2, normed_one, c0, c1, c2, c3, v0, v1, v2, v3, dz, low, out, sums, spread, cots
):
    t = place[0]
    fill((v0, v1, v2, v3), spread, t)
    width = c0.shape[1]
    r = dz.shape[0]
    for k, ref in enumerate((c0, c1, c2, c3)):
        cots[:, block(t ^ k, width)] = ref[sequence * r : (sequence + 1) * r, :].astype(F32)
    h_one = normed_one[...] * spread[1:2, :] + spread[2:3, :]
    z = h_one + (s0[...].astype(F32) + s1[...].astype(F32) + s2[...].astype(F32)) + spread[3:4, :]
    normed, inverse = normed_of(z)
    out[...] = (normed * spread[4:5, :] + spread[5:6, :]).astype(BF)
    grad = cots[...]
    sums[0:1, :] = jnp.sum(grad * normed, axis=0, keepdims=True)
    sums[1:2, :] = jnp.sum(grad, axis=0, keepdims=True)
    back = norm_back(grad * spread[4:5, :], normed, inverse)
    sums[2:3, :] = jnp.sum(back, axis=0, keepdims=True)
    dz[...] = back
    low[...] = back.astype(BF)


def first_back_kernel(place, s0, s1, s2, dz, normed_ref, inverse_ref, v0, v1, v2, v3, low, sums, spread):
    fill((v0, v1, v2, v3), spread, place[0])
    dh = dz[...] + (s0[...].astype(F32) + s1[...].astype(F32) + s2[...].astype(F32))
    normed = normed_ref[...]
    sums[0:1, :] = jnp.sum(dh * normed, axis=0, keepdims=True)
    sums[1:2, :] = jnp.sum(dh, axis=0, keepdims=True)
    back = norm_back(dh * spread[1:2, :], normed, inverse_ref[...])
    sums[2:3, :] = jnp.sum(back, axis=0, keepdims=True)
    low[...] = back.astype(BF)


def feed_kernel(place, h0, h1, w_in, b_in, w_down, hidden, slope, keep, send):
    rows = jnp.concatenate([h0[...], h1[...]], axis=0)
    r = h0.shape[0]
    units = w_in.shape[1]
    step = min(256, units)
    total = jnp.zeros((2 * r, w_down.shape[1]), F32)
    for first in range(0, units, step):
        here = slice(first, first + step)
        pre_act = mm(rows, w_in[:, here]) + b_in[here].astype(F32)[None, :]
        cdf = 0.5 * (1.0 + lax.erf(pre_act * (2.0**-0.5)))
        rise = pre_act * jnp.exp(-0.5 * pre_act * pre_act) * ((2.0 * math.pi) ** -0.5)
        active = (pre_act * cdf).astype(BF)
        hidden[:, here] = active
        slope[:, here] = (cdf + rise).astype(BF)
        total = total + mm(active, w_down[here, :])
    keep[...] = total[:r].astype(BF)
    send[...] = total[r:].astype(BF)


def feed_back_kernel(place, d0, d1, slope, w_down, w_in, dpre, keep, send, bias):
    rows = jnp.concatenate([d0[...], d1[...]], axis=0)
    r = d0.shape[0]
    units = w_in.shape[1]
    step = min(256, units)
    total = jnp.zeros((2 * r, w_in.shape[0]), F32)
    for first in range(0, units, step):
        here = slice(first, first + step)
        grad = (against(rows, w_down[here, :]) * slope[:, here].astype(F32)).astype(BF)
        dpre[:, here] = grad
        bias[:, here] = jnp.sum(grad.astype(F32), axis=0, keepdims=True)
        total = total + against(grad, w_in[:, here])
    keep[...] = total[:r].astype(BF)
    send[...] = total[r:].astype(BF)


def weight_grad_kernel(groups, stacked, bit, place, *refs):
    keep, send = refs[-2:]
    set_bit = jnp.where((place[1] & bit) == 0, 0, 1)
    lefts, rights = [], []
    at = 0
    for left, right in groups:
        lefts.append(refs[at : at + left])
        rights.append(refs[at + left : at + left + right])
        at += left + right

    def joined(parts, columns):
        parts = [p[:, columns] for p in parts]
        return parts[0] if len(parts) == 1 else jnp.concatenate(parts, axis=0)

    half, width = keep.shape
    step = min(256, half)
    for half_index, out in ((1 - set_bit, send), (set_bit, keep)):
        for first in range(0, half, step):
            here = block(half_index * (half // step) + first // step, step)
            if stacked:
                terms = [over_rows(joined(l, slice(None)), joined(r, here)) for l, r in zip(lefts, rights)]
            else:
                terms = [over_rows(joined(l, here), joined(r, slice(None))) for l, r in zip(lefts, rights)]
            out[first : first + step, :] = total_of(terms).astype(BF)


def weight_grad(line, pairs, height, width, bit, name, stacked=False):
    operands = [x for left, right in pairs for x in (*left, *right)]
    groups = [(len(left), len(right)) for left, right in pairs]
    depth = sum(x.shape[0] for left, _ in pairs for x in left)
    return line(
        functools.partial(weight_grad_kernel, groups, stacked, bit),
        name,
        [((height // 2, width), BF)] * 2,
        operands,
        flops=2 * depth * height * width,
    )


def proj_grad_kernel(count, bits, place, *refs):
    t = place[0]
    out_keep, out_send, packed = refs[8 + count : 11 + count]
    outs, full = refs[-5:-1], refs[-1]
    size = refs[0].shape[1]
    rows = refs[0].shape[0]
    for k in range(4):
        terms = [over_rows(refs[k][...], refs[8][...])]
        for i in range(1, count):
            terms.append(over_rows(refs[4 + k][(i - 1) * rows : i * rows, :], refs[8 + i][...]))
        full[block(t ^ k, size), :] = total_of(terms).astype(BF)
    half = outs[0].shape[0]
    outs[2][half:, :] = packed[...]
    outs[3][half:, :] = packed[...]
    for j, bit in enumerate(bits):
        set_bit = jnp.where((place[1] & bit) == 0, 0, 1)
        columns = slice(j * size, (j + 1) * size)
        to = slice((j % 2) * size, (j % 2 + 1) * size)
        outs[2 * (j // 2)][:half, to] = full[block(set_bit, half), columns]
        outs[2 * (j // 2) + 1][:half, to] = full[block(1 - set_bit, half), columns]
    outs[2][:half, size:] = out_keep[...]
    outs[3][:half, size:] = out_send[...]


def halve_kernel(bit, extra, place, kept, got, keep, send):
    set_bit = jnp.where((place[1] & bit) == 0, 0, 1)
    half = keep.shape[0] - extra
    for index, out in ((1 - set_bit, send), (set_bit, keep)):
        here = block(index, half)
        out[:half, :] = (kept[here, :].astype(F32) + got[here, :].astype(F32)).astype(BF)
        if extra:
            out[half:, :] = (kept[2 * half :, :].astype(F32) + got[2 * half :, :].astype(F32)).astype(BF)


def add_kernel(place, kept, got, out, *rest):
    half = out.shape[0]
    out[...] = (kept[:half, :].astype(F32) + got[:half, :].astype(F32)).astype(BF)
    for ref in rest:
        ref[...] = kept[half:, :].astype(F32) + got[half:, :].astype(F32)


def join_kernel(bit, place, mine, got, out):
    set_bit = jnp.where((place[1] & bit) == 0, 0, 1)
    half = mine.shape[0]
    for index, ref in ((set_bit, mine), (1 - set_bit, got)):
        out[block(index, half), :] = ref[...].astype(out.dtype)


def split_kernel(unstack):
    def shapes(height, width):
        return [((height, width // 2), F32), (unstack or (height, width // 2), F32)]

    def kernel(bit, place, mine, got, one, two):
        set_bit = jnp.where((place[1] & bit) == 0, 0, 1)
        half = mine.shape[0]
        size = one.shape[1]
        for index, ref in ((set_bit, mine), (1 - set_bit, got)):
            one[block(index, half), :] = ref[:, :size].astype(F32)
            if unstack:
                tall = unstack[0]
                for j in range(half // tall):
                    columns = block(index * (half // tall) + j, size)
                    two[:, columns] = ref[j * tall : (j + 1) * tall, size:].astype(F32)
            else:
                two[block(index, half), :] = ref[:, size:].astype(F32)

    return shapes, kernel


def whole_shapes(height, width):
    return [((height, width), F32)]


def dp_sum(line, keep, send, bits, name, last=(whole_shapes, join_kernel), extra=0):
    got = swap(send, "dp", bits[0])
    yield
    half, width = keep.shape
    half -= extra
    for bit in bits[1:]:
        half //= 2
        keep, send = line(
            functools.partial(halve_kernel, bit, extra),
            name + "_halve",
            [((half + extra, width), BF)] * 2,
            [keep, got],
        )
        got = swap(send, "dp", bit)
        yield
    mine, *rest = line(
        add_kernel, name + "_add", [((half, width), BF)] + [((extra, width), F32)] * (extra > 0), [keep, got]
    )
    got = swap(mine, "dp", bits[-1])
    yield
    for bit in reversed(bits[1:]):
        half *= 2
        (mine,) = line(
            functools.partial(join_kernel, bit), name + "_join", [((half, width), BF)], [mine, got]
        )
        got = swap(mine, "dp", bits[bits.index(bit) - 1])
        yield
    shapes, kernel = last
    whole = line(
        functools.partial(kernel, bits[0]), name + "_whole", shapes(2 * half, width), [mine, got]
    )
    return [*whole, *rest]


class Steps:
    def __init__(self, generator):
        self.generator = generator
        self.result = None
        self.go()

    def go(self, times=1):
        for _ in range(times):
            if self.result is None:
                try:
                    next(self.generator)
                except StopIteration as stop:
                    self.result = stop.value

    def finish(self):
        while self.result is None:
            self.go()
        return self.result


def small_pack_kernel(count, place, *refs):
    out = refs[-1]
    width = out.shape[1] // 2
    b_in = total_of([ref[...] for ref in refs[4 : 4 + 2 * count]])
    b_proj = total_of([ref[...] for ref in refs[4 + 2 * count : 4 + 3 * count]])
    features = total_of([ref[...] for ref in refs[:4]])
    rows = [features[i : i + 1, :] for i in range(6)]
    for whole in (b_in, b_proj):
        rows += [whole[:, j * width : (j + 1) * width] for j in range(whole.shape[1] // width)]
    rows += [jnp.zeros((1, width), F32)] * (2 * out.shape[0] - len(rows))
    left, right = jnp.concatenate(rows[0::2], axis=0), jnp.concatenate(rows[1::2], axis=0)
    out[...] = jnp.concatenate([left, right], axis=1).astype(BF)


def small_out_kernel(place, total, *outs):
    width = total.shape[1] // 2
    row = 0
    for out in outs:
        for j in range(out.shape[0] // width):
            out[j * width : (j + 1) * width] = total[row // 2, (row % 2) * width : (row % 2 + 1) * width]
            row += 1


def out_pack_kernel(count, place, *refs):
    t = place[0]
    r = refs[0].shape[0]
    for k, out in enumerate(refs[count:]):
        for i in range(count):
            out[i * r : (i + 1) * r, :] = refs[i][:, block(t ^ k, out.shape[1])]


def rows_kernel(count, place, *refs):
    t = place[0]
    out = refs[-1]
    r = refs[0].shape[0] // count
    for k in range(4):
        for i in range(count):
            out[block(4 * i + (t ^ k), r), :] = refs[k][i * r : (i + 1) * r, :]


def tokens_kernel(place, *refs):
    out = refs[-1]
    r = refs[0].shape[0]
    for i in range((len(refs) - 1) // 4):
        terms = [first_of(refs[4 * i + j]) for j in range(4)]
        out[i * r : (i + 1) * r, :] = total_of(terms).astype(BF)


def pack_kernel(count, place, *refs):
    t = place[0]
    outs, spread = refs[2 * count : 2 * count + 4], refs[-1]
    spread[0:3, :] = total_of([refs[i][...] for i in range(count)])
    spread[3:6, :] = total_of([refs[count + i][...] for i in range(count)])
    width = outs[0].shape[1]
    for k, ref in enumerate(outs):
        ref[...] = spread[0:6, block(t ^ k, width)]


def total_of(parts):
    return functools.reduce(lambda a, b: a + b, parts)


def local(
    tokens,
    segment_ids,
    w_query,
    w_key,
    w_value,
    b_query,
    b_value,
    w_out,
    b_out,
    gain_one,
    bias_one,
    w_in,
    b_in,
    w_down,
    b_down,
    gain_two,
    bias_two,
    cotangent,
):
    t = lax.axis_index("tensor")
    d = lax.axis_index("dp")
    line = Line(jnp.stack([t, d]).astype(jnp.int32))
    row_count, cols = tokens.shape
    width = w_query.shape[0]
    units = w_in.shape[1]
    count = row_count // LEN
    r = LEN // 4
    heads = cols // HD
    labels = segment_ids.reshape(count, 1, LEN)
    every = range(count)
    spread = pltpu.VMEM((8, width), F32)

    first, rest = tokens[:LEN], tokens[LEN:]
    rest_across = swap(rest, "tensor", 2)
    pieces = [gather_blocks(first)]

    def onward(kept, got, pair):
        (both,) = line(
            second_of_onward_kernel if pair else onward_kernel,
            "onward",
            [(kept.shape[1:] if pair else kept.shape, BF)],
            [kept, got],
        )
        return swap(both, "tensor", 2)

    ctxs, projs, totals, attn_terms = [], [], [], []

    def do_attend(i):
        proj, ctx, total, residual, keep, send = line(
            functools.partial(attend_kernel, max(i - 1, 0)),
            "attend",
            [
                ((LEN, 3 * cols), BF),
                ((LEN, cols), BF),
                ((LEN, heads), F32),
                ((r, width), BF),
                ((2, r, width), BF),
                ((2, r, width), BF),
            ],
            [*pieces[min(i, 1)], w_query, w_key, w_value, b_query, b_value, labels[i], w_out],
            flops=2 * LEN * width * 4 * cols + 4 * LEN * LEN * cols * heads,
            exps=heads * LEN * LEN,
        )
        attn_terms.append((keep, swap(send, "tensor", 1), residual))
        projs.append(proj)
        ctxs.append(ctx)
        totals.append(total)

    def do_attend_onward(i):
        keep, sent, residual = attn_terms[i]
        attn_terms[i] = [keep, sent, onward(keep, sent, True), residual]

    firsts, h_pieces = [], []

    def do_first_norm(i):
        normed, inverse, low = line(
            first_norm_kernel,
            "first_norm",
            [((r, width), F32), ((r, 1), F32), ((r, width), BF)],
            [*attn_terms[i], *vectors],
            flops=20 * r * width,
            scratch=[spread],
        )
        firsts.append((normed, inverse))
        h_pieces.append(gather_blocks(low))

    feeds = {}

    def do_feed(i, j):
        feeds[i, j] = line(
            feed_kernel,
            "feed",
            [((2 * r, units), BF), ((2 * r, units), BF), ((r, width), BF), ((r, width), BF)],
            [*h_pieces[i][2 * j : 2 * j + 2], w_in, b_in, w_down],
            flops=8 * r * width * units,
            exps=2 * r * units * 2,
        )

    seconds, dz_pieces, results = [], [], []

    def do_second_norm(i):
        dz, low, result, sums = line(
            functools.partial(second_norm_kernel, i),
            "second_norm",
            [((r, width), F32), ((r, width), BF), ((r, width), BF), ((3, width), F32)],
            [
                *feed_terms[i],
                firsts[i][0],
                *cots,
                *vectors,
            ],
            flops=40 * r * width,
            scratch=[spread, pltpu.VMEM((r, width), F32)],
        )
        seconds.append((dz, sums))
        results.append(result)
        dz_pieces.append(gather_blocks(low))

    backs = {}

    def do_feed_back(i, j):
        backs[i, j] = line(
            feed_back_kernel,
            "feed_back",
            [((2 * r, units), BF), ((r, width), BF), ((r, width), BF), ((1, units), F32)],
            [*dz_pieces[i][2 * j : 2 * j + 2], feeds[i, j][1], w_down, w_in],
            flops=8 * r * width * units,
        )

    thirds, dz1_pieces = [], []

    def do_first_back(i):
        low, sums = line(
            first_back_kernel,
            "first_back",
            [((r, width), BF), ((3, width), F32)],
            [*back_terms[i], seconds[i][0], *firsts[i], *vectors],
            flops=30 * r * width,
            scratch=[spread],
        )
        thirds.append(sums)
        dz1_pieces.append(gather_blocks(low))

    dprojs, token_terms, b_proj_parts = [], [], []

    def do_attend_back(i):
        dproj, keep, send, dz_cols, bias = line(
            attend_back_kernel,
            "attend_back",
            [
                ((LEN, 3 * cols), BF),
                ((2, LEN, cols), BF),
                ((2, LEN, cols), BF),
                ((LEN, cols), BF),
                ((1, 3 * cols), F32),
            ],
            [*dz1_pieces[i], w_out, projs[i], totals[i], labels[i], w_query, w_key, w_value],
            flops=2 * LEN * width * 4 * cols + 10 * LEN * LEN * cols * heads,
            exps=heads * LEN * LEN,
            scratch=[pltpu.VMEM((LEN, cols), BF)],
        )
        token_terms.append((dz_cols, keep, swap(send, "tensor", 1)))
        dprojs.append(dproj)
        b_proj_parts.append(bias)

    def do_tokens_onward(i):
        dz_cols, keep, sent = token_terms[i]
        token_terms[i] = [dz_cols, keep, sent, onward(keep, sent, True)]

    feed_terms, back_terms = {}, {}

    def send_beside(terms, i, b0, b1, b2, b3):
        terms[i] = (b0, swap(b1, "tensor", 1), b2, swap(b3, "tensor", 1))

    def send_across(terms, i):
        b0, near, b2, far = terms[i]
        terms[i] = (b0, near, onward(b2, far, False))

    def staggered(first, second):
        for i in every:
            first(i)
            if i:
                second(i - 1)

    do_attend(0)
    (vectors,) = line(
        vectors_kernel, "vectors", [((6, cols), BF)], [b_out, gain_one, bias_one, b_down, gain_two, bias_two]
    )
    vectors = gather_blocks(vectors)
    cots = exchange_blocks(
        line(
            functools.partial(cot_pack_kernel, count), "cot_pack", [((count * r, cols), BF)] * 4, [cotangent]
        )
    )
    rest_across = line.after(rest_across)
    pieces.append((rest, swap(rest, "tensor", 1), rest_across, swap(rest_across, "tensor", 1)))
    for i in every[1:]:
        do_attend(i)
        do_attend_onward(i - 1)
        if i == 1:
            line.take(*cots)
    do_attend_onward(count - 1)

    for i in every:
        do_first_norm(i)
        do_feed(i, 0)

    def second_feed(i):
        do_feed(i, 1)
        send_beside(feed_terms, i, *feeds[i, 0][2:], *feeds[i, 1][2:])

    staggered(second_feed, lambda i: send_across(feed_terms, i))
    send_across(feed_terms, count - 1)
    for i in every:
        do_second_norm(i)
        do_feed_back(i, 0)

    early, late = dp_bits(0), dp_bits(1)

    def second_back(i):
        do_feed_back(i, 1)
        send_beside(back_terms, i, *backs[i, 0][1:3], *backs[i, 1][1:3])

    for i in every[:-1]:
        second_back(i)
        if i:
            send_across(back_terms, i - 1)
    down_pairs = [
        ([feeds[i, j][0]], dz_pieces[i][2 * j : 2 * j + 2]) for i in every for j in range(2)
    ]
    down = Steps(
        dp_sum(line, *weight_grad(line, down_pairs, units, width, early[0], "down_grad"), early, "down")
    )
    for i in every[-2:-1]:
        send_across(back_terms, i)
    second_back(count - 1)
    in_pairs = [
        (h_pieces[i][2 * j : 2 * j + 2], [backs[i, j][0]]) for i in every for j in range(2)
    ]
    into = Steps(
        dp_sum(line, *weight_grad(line, in_pairs, width, units, late[0], "in_grad"), late, "into")
    )
    send_across(back_terms, count - 1)
    for i in every[:-1]:
        do_first_back(i)
    down.go()
    do_first_back(count - 1)
    pieces_out = exchange_blocks(
        line(
            functools.partial(out_pack_kernel, count),
            "out_pack",
            [((count * r, cols), BF)] * 4,
            results,
        )
    )
    wide = exchange_blocks(
        line(
            functools.partial(pack_kernel, count),
            "pack",
            [((6, cols), F32)] * 4,
            [s for _, s in seconds] + thirds,
            scratch=[spread],
        )
    )

    into.go()
    do_attend_back(0)
    down.go()
    for i in every[1:]:
        do_attend_back(i)
        do_tokens_onward(i - 1)
        (into if i == 1 else down).go()
    out_pairs = [([ctxs[i]], [dz1_pieces[i][k] for k in range(4)]) for i in every]
    out_half = weight_grad(line, out_pairs, width, cols, late[0], "out_grad", stacked=True)
    do_tokens_onward(count - 1)
    extra = -(-(6 + units // cols + 3) // 32) * 16
    (packed,) = line(
        functools.partial(small_pack_kernel, count),
        "small_pack",
        [((extra, 2 * cols), BF)],
        [*wide, *[b[3] for b in backs.values()], *b_proj_parts],
    )
    half_shape = ((width // 2, 2 * cols), BF)
    more_shape = ((width // 2 + extra, 2 * cols), BF)
    first_half = line(
        functools.partial(proj_grad_kernel, count, (early[0], early[0], late[0])),
        "proj_grad",
        [half_shape, half_shape, more_shape, more_shape],
        [*pieces[0], *pieces[1], *dprojs, *out_half, packed],
        flops=2 * row_count * width * 3 * cols,
        scratch=[pltpu.VMEM((width, 3 * cols), BF)],
    )
    query_key = Steps(dp_sum(line, first_half[0], first_half[1], early, "query_key", split_kernel(None)))
    value_out = Steps(
        dp_sum(line, first_half[2], first_half[3], late, "value_out", split_kernel((cols, width)), extra)
    )
    into.go()
    down.go()
    (result,) = line(
        functools.partial(rows_kernel, count), "out_rows", [((row_count, cols), BF)], pieces_out
    )
    query_key.go()
    value_out.go()
    down.go()
    into.go()
    (grad_tokens,) = line(
        tokens_kernel, "token_rows", [((row_count, cols), BF)], [x for terms in token_terms for x in terms]
    )
    query_key.go()
    value_out.go()
    into.go()
    query_key.go()
    value_out.go()
    down.go()
    waiting = [query_key, value_out, into, down]
    while any(s.result is None for s in waiting):
        for s in waiting:
            s.go()
    sums = line(
        small_out_kernel,
        "small_out",
        [((s,), F32) for s in [cols] * 6 + [units] + [cols] * 3],
        [value_out.result[2]],
    )

    return (
        result,
        grad_tokens,
        query_key.result[0],
        query_key.result[1],
        value_out.result[0],
        sums[7],
        sums[9],
        value_out.result[1],
        sums[5],
        sums[3],
        sums[4],
        into.result[0],
        sums[6],
        down.result[0],
        sums[2],
        sums[0],
        sums[1],
    )


def solution(mesh):
    placed = (
        P("dp", "tensor"),
        P("dp"),
        P(None, "tensor"),
        P(None, "tensor"),
        P(None, "tensor"),
        P("tensor"),
        P("tensor"),
        P("tensor", None),
        P("tensor"),
        P("tensor"),
        P("tensor"),
        P(None, "tensor"),
        P("tensor"),
        P("tensor", None),
        P("tensor"),
        P("tensor"),
        P("tensor"),
        P("dp", "tensor"),
    )
    return jax.shard_map(
        local,
        mesh=mesh,
        in_specs=placed,
        out_specs=(
            P("dp", "tensor"),
            P("dp", "tensor"),
            P(None, "tensor"),
            P(None, "tensor"),
            P(None, "tensor"),
            P("tensor"),
            P("tensor"),
            P("tensor", None),
            P("tensor"),
            P("tensor"),
            P("tensor"),
            P(None, "tensor"),
            P("tensor"),
            P("tensor", None),
            P("tensor"),
            P("tensor"),
            P("tensor"),
        ),
        check_vma=False,
    )
```

```python
import functools
import math

import jax
import jax.numpy as jnp
from jax import lax
from jax.experimental import pallas as pl
from jax.experimental.pallas import tpu as pltpu
from jax.sharding import PartitionSpec as P

HD = 64
LEN = 512

EPSILON = 1e-05
MASKED = -1000000000.0
VMEM_LIMIT = 8 << 20
BF = jnp.bfloat16
F32 = jnp.float32


def mm(left, right):
    return lax.dot_general(left, right, (((1,), (0,)), ((), ())), preferred_element_type=F32)


def over_rows(left, right):
    return lax.dot_general(left, right, (((0,), (0,)), ((), ())), preferred_element_type=F32)


def against(left, right):
    return lax.dot_general(left, right, (((1,), (1,)), ((), ())), preferred_element_type=F32)


def swap(values, axis, bit):
    size = lax.axis_size(axis)
    return lax.ppermute(values, axis, [(i, i ^ bit) for i in range(size)])


def gather_blocks(own):
    across = swap(own, "tensor", 2)
    beside = swap(own, "tensor", 1)
    corner = swap(across, "tensor", 1)
    return own, beside, across, corner


def exchange_blocks(blocks):
    return (
        blocks[0],
        swap(blocks[1], "tensor", 1),
        swap(blocks[2], "tensor", 2),
        swap(blocks[3], "tensor", 3),
    )


def dp_bits(order):
    size = lax.axis_size("dp")
    bits = [1 << i for i in range(int(math.log2(size)))]
    if order and len(bits) > 1:
        bits[0], bits[1] = bits[1], bits[0]
    return bits


class Line:
    def __init__(self, place):
        self.place = place

    def __call__(self, kernel, name, out_shape, operands, flops=0, exps=0, scratch=()):
        out_shape = [jax.ShapeDtypeStruct(s, d) for s, d in out_shape]
        size = sum(math.prod(o.shape) * o.dtype.itemsize for o in list(operands) + out_shape)
        whole = pl.BlockSpec(memory_space=pltpu.VMEM)
        outs = pl.pallas_call(
            kernel,
            in_specs=[pl.BlockSpec(memory_space=pltpu.SMEM)] + [whole] * len(operands),
            out_specs=[whole] * len(out_shape),
            out_shape=out_shape,
            scratch_shapes=list(scratch),
            compiler_params=pltpu.CompilerParams(vmem_limit_bytes=VMEM_LIMIT),
            cost_estimate=pl.CostEstimate(flops=flops, transcendentals=exps, bytes_accessed=size),
            name=name,
        )(self.place, *operands)
        last = min(outs, key=lambda o: math.prod(o.shape))
        self.place, _ = lax.optimization_barrier((self.place, last))
        return outs

    def after(self, value):
        return lax.optimization_barrier((value, self.place))[0]

    def take(self, *values):
        self.place = lax.optimization_barrier((self.place, *values))[0]


def block(index, size):
    return pl.ds(pl.multiple_of(index * size, size), size)


def first_of(ref):
    return (ref[0] if len(ref.shape) == 3 else ref[...]).astype(F32)


def head_lanes(width, head):
    lane = lax.broadcasted_iota(jnp.int32, (1, width), 1)
    return (lane >= head * HD) & (lane < (head + 1) * HD)


def allowed_block(label_row):
    length = label_row.shape[1]
    label_row = label_row.astype(F32)
    label_column = jnp.transpose(jnp.broadcast_to(label_row, (8, length)))[:, :1]
    same = label_column == label_row
    diagonal = lax.broadcasted_iota(jnp.int32, (length, length), 0) == lax.broadcasted_iota(
        jnp.int32, (length, length), 1
    )
    return same & ((label_column != 0.0) | diagonal)


def attend_kernel(
    sequence, place, p0, p1, p2, p3, wq, wk, wv, bq, bv, label, w_out, proj, ctx, total, residual, keep, send
):
    t = place[0]
    width = wq.shape[1]
    length = ctx.shape[0]
    rows = length // 4
    pieces = [p.at[sequence * length : (sequence + 1) * length, :] for p in (p0, p1, p2, p3)]
    for k, piece in enumerate(pieces):
        residual[:, block(t ^ k, width)] = piece[block(t, rows), :]
    parts = []
    for weight in (wq, wk, wv):
        parts.append(total_of([mm(piece[...], weight[block(t ^ k, width), :]) for k, piece in enumerate(pieces)]))
    queries = (parts[0] + bq[...].astype(F32)[None, :]).astype(BF)
    keys = parts[1].astype(BF)
    values = (parts[2] + bv[...].astype(F32)[None, :]).astype(BF)
    proj[:, :width] = queries
    proj[:, width : 2 * width] = keys
    proj[:, 2 * width :] = values
    allowed = allowed_block(label[...])
    context = jnp.zeros(queries.shape, F32)
    zero = jnp.zeros((), BF)
    for head in range(width // HD):
        lanes = head_lanes(width, head)
        scores = against(jnp.where(lanes, queries, zero), keys) * (HD**-0.5)
        scores = jnp.where(allowed, scores, MASKED)
        peak = jnp.max(scores, axis=1, keepdims=True)
        terms = jnp.exp(scores - peak)
        summed = jnp.sum(terms, axis=1, keepdims=True)
        probs = (terms / summed).astype(BF)
        context = context + mm(probs, jnp.where(lanes, values, zero))
        total[:, head : head + 1] = peak + jnp.log(summed)
    context = context.astype(BF)
    for j in range(4):
        ctx[block(t ^ j, rows), :] = context[j * rows : (j + 1) * rows]
    for k in range(4):
        part = mm(ctx[k * rows : (k + 1) * rows, :], w_out[...]).astype(BF)
        (send if k % 2 else keep)[k // 2] = part


def attend_back_kernel(
    place, d0, d1, d2, d3, w_out, proj, total, label, wq, wk, wv, dproj, keep, send, dz_cols, bias, dctx
):
    t = place[0]
    width = wq.shape[1]
    rows = d0.shape[0]
    for k, piece in enumerate((d0, d1, d2, d3)):
        dctx[block(t ^ k, rows), :] = against(piece[...], w_out[...]).astype(BF)
        dz_cols[block(t ^ k, rows), :] = piece[:, block(t, width)]
    allowed = allowed_block(label[...])
    queries, keys, values = proj[:, :width], proj[:, width : 2 * width], proj[:, 2 * width :]
    dcontext = dctx[...]
    scale = HD**-0.5
    dquery = jnp.zeros(queries.shape, F32)
    dkey = jnp.zeros(queries.shape, F32)
    dvalue = jnp.zeros(queries.shape, F32)
    zero = jnp.zeros((), BF)
    for head in range(width // HD):
        lanes = head_lanes(width, head)
        q_head = jnp.where(lanes, queries, zero)
        d_head = jnp.where(lanes, dcontext, zero)
        k_head = jnp.where(lanes, keys, zero)
        scores = against(q_head, keys) * scale
        scores = jnp.where(allowed, scores, MASKED)
        probs = jnp.exp(scores - total[:, head : head + 1])
        dprobs = against(d_head, values)
        delta = jnp.sum(probs * dprobs, axis=1, keepdims=True)
        dscores = (probs * (dprobs - delta)).astype(BF)
        dquery = dquery + mm(dscores, k_head)
        dkey = dkey + over_rows(dscores, q_head)
        dvalue = dvalue + over_rows(probs.astype(BF), d_head)
    grads = ((dquery * scale).astype(BF), (dkey * scale).astype(BF), dvalue.astype(BF))
    for i, grad in enumerate(grads):
        dproj[:, i * width : (i + 1) * width] = grad
        bias[:, i * width : (i + 1) * width] = jnp.sum(grad.astype(F32), axis=0, keepdims=True)
    for k in range(4):
        here = block(t ^ k, width)
        part = total_of([against(grad, weight[here, :]) for grad, weight in zip(grads, (wq, wk, wv))])
        (send if k % 2 else keep)[k // 2] = part.astype(BF)


def normed_of(values):
    center = values - jnp.mean(values, axis=1, keepdims=True)
    inverse = lax.rsqrt(jnp.mean(center * center, axis=1, keepdims=True) + EPSILON)
    return center * inverse, inverse


def norm_back(scaled, normed, inverse):
    mean = jnp.mean(scaled, axis=1, keepdims=True)
    along = jnp.mean(scaled * normed, axis=1, keepdims=True)
    return inverse * (scaled - mean - normed * along)


def fill(vectors, spread, t):
    width = vectors[0].shape[1]
    for k, ref in enumerate(vectors):
        spread[0:6, block(t ^ k, width)] = ref[...].astype(F32)


def onward_kernel(place, kept, got, out):
    out[...] = (kept[...].astype(F32) + got[...].astype(F32)).astype(BF)


def second_of_onward_kernel(place, kept, got, out):
    out[...] = (kept[1].astype(F32) + got[1].astype(F32)).astype(BF)


def vectors_kernel(place, *refs):
    for i, ref in enumerate(refs[:-1]):
        refs[-1][i : i + 1, :] = ref[...][None, :]


def first_norm_kernel(place, s0, s1, s2, residual, v0, v1, v2, v3, normed_ref, inverse_ref, low, spread):
    fill((v0, v1, v2, v3), spread, place[0])
    z = first_of(s0) + first_of(s1) + first_of(s2)
    z = residual[...].astype(F32) + z + spread[0:1, :]
    normed, inverse = normed_of(z)
    normed_ref[...] = normed
    inverse_ref[...] = inverse
    low[...] = (normed * spread[1:2, :] + spread[2:3, :]).astype(BF)


def cot_pack_kernel(count, place, cot, *outs):
    t = place[0]
    r = outs[0].shape[0] // count
    for k, out in enumerate(outs):
        for i in range(count):
            out[i * r : (i + 1) * r, :] = cot[block(4 * i + (t ^ k), r), :]


def second_norm_kernel(
    sequence, place, s0, s1, s2, normed_one, c0, c1, c2, c3, v0, v1, v2, v3, dz, low, out, sums, spread, cots
):
    t = place[0]
    fill((v0, v1, v2, v3), spread, t)
    width = c0.shape[1]
    r = dz.shape[0]
    for k, ref in enumerate((c0, c1, c2, c3)):
        cots[:, block(t ^ k, width)] = ref[sequence * r : (sequence + 1) * r, :].astype(F32)
    h_one = normed_one[...] * spread[1:2, :] + spread[2:3, :]
    z = h_one + (s0[...].astype(F32) + s1[...].astype(F32) + s2[...].astype(F32)) + spread[3:4, :]
    normed, inverse = normed_of(z)
    out[...] = (normed * spread[4:5, :] + spread[5:6, :]).astype(BF)
    grad = cots[...]
    sums[0:1, :] = jnp.sum(grad * normed, axis=0, keepdims=True)
    sums[1:2, :] = jnp.sum(grad, axis=0, keepdims=True)
    back = norm_back(grad * spread[4:5, :], normed, inverse)
    sums[2:3, :] = jnp.sum(back, axis=0, keepdims=True)
    dz[...] = back
    low[...] = back.astype(BF)


def first_back_kernel(place, s0, s1, s2, dz, normed_ref, inverse_ref, v0, v1, v2, v3, low, sums, spread):
    fill((v0, v1, v2, v3), spread, place[0])
    dh = dz[...] + (s0[...].astype(F32) + s1[...].astype(F32) + s2[...].astype(F32))
    normed = normed_ref[...]
    sums[0:1, :] = jnp.sum(dh * normed, axis=0, keepdims=True)
    sums[1:2, :] = jnp.sum(dh, axis=0, keepdims=True)
    back = norm_back(dh * spread[1:2, :], normed, inverse_ref[...])
    sums[2:3, :] = jnp.sum(back, axis=0, keepdims=True)
    low[...] = back.astype(BF)


def feed_kernel(place, h0, h1, w_in, b_in, w_down, hidden, slope, keep, send):
    rows = jnp.concatenate([h0[...], h1[...]], axis=0)
    r = h0.shape[0]
    units = w_in.shape[1]
    step = min(256, units)
    total = jnp.zeros((2 * r, w_down.shape[1]), F32)
    for first in range(0, units, step):
        here = slice(first, first + step)
        pre_act = mm(rows, w_in[:, here]) + b_in[here].astype(F32)[None, :]
        cdf = 0.5 * (1.0 + lax.erf(pre_act * (2.0**-0.5)))
        rise = pre_act * jnp.exp(-0.5 * pre_act * pre_act) * ((2.0 * math.pi) ** -0.5)
        active = (pre_act * cdf).astype(BF)
        hidden[:, here] = active
        slope[:, here] = (cdf + rise).astype(BF)
        total = total + mm(active, w_down[here, :])
    keep[...] = total[:r].astype(BF)
    send[...] = total[r:].astype(BF)


def feed_back_kernel(place, d0, d1, slope, w_down, w_in, dpre, keep, send, bias):
    rows = jnp.concatenate([d0[...], d1[...]], axis=0)
    r = d0.shape[0]
    units = w_in.shape[1]
    step = min(256, units)
    total = jnp.zeros((2 * r, w_in.shape[0]), F32)
    for first in range(0, units, step):
        here = slice(first, first + step)
        grad = (against(rows, w_down[here, :]) * slope[:, here].astype(F32)).astype(BF)
        dpre[:, here] = grad
        bias[:, here] = jnp.sum(grad.astype(F32), axis=0, keepdims=True)
        total = total + against(grad, w_in[:, here])
    keep[...] = total[:r].astype(BF)
    send[...] = total[r:].astype(BF)


def weight_grad_kernel(groups, stacked, bit, place, *refs):
    keep, send = refs[-2:]
    set_bit = jnp.where((place[1] & bit) == 0, 0, 1)
    lefts, rights = [], []
    at = 0
    for left, right in groups:
        lefts.append(refs[at : at + left])
        rights.append(refs[at + left : at + left + right])
        at += left + right

    def joined(parts, columns):
        parts = [p[:, columns] for p in parts]
        return parts[0] if len(parts) == 1 else jnp.concatenate(parts, axis=0)

    half, width = keep.shape
    step = min(256, half)
    for half_index, out in ((1 - set_bit, send), (set_bit, keep)):
        for first in range(0, half, step):
            here = block(half_index * (half // step) + first // step, step)
            if stacked:
                terms = [over_rows(joined(l, slice(None)), joined(r, here)) for l, r in zip(lefts, rights)]
            else:
                terms = [over_rows(joined(l, here), joined(r, slice(None))) for l, r in zip(lefts, rights)]
            out[first : first + step, :] = total_of(terms).astype(BF)


def weight_grad(line, pairs, height, width, bit, name, stacked=False):
    operands = [x for left, right in pairs for x in (*left, *right)]
    groups = [(len(left), len(right)) for left, right in pairs]
    depth = sum(x.shape[0] for left, _ in pairs for x in left)
    return line(
        functools.partial(weight_grad_kernel, groups, stacked, bit),
        name,
        [((height // 2, width), BF)] * 2,
        operands,
        flops=2 * depth * height * width,
    )


def proj_grad_kernel(count, bits, place, *refs):
    t = place[0]
    out_keep, out_send, packed = refs[8 + count : 11 + count]
    outs, full = refs[-5:-1], refs[-1]
    size = refs[0].shape[1]
    rows = refs[0].shape[0]
    for k in range(4):
        terms = [over_rows(refs[k][...], refs[8][...])]
        for i in range(1, count):
            terms.append(over_rows(refs[4 + k][(i - 1) * rows : i * rows, :], refs[8 + i][...]))
        full[block(t ^ k, size), :] = total_of(terms).astype(BF)
    half = outs[0].shape[0]
    outs[2][half:, :] = packed[...]
    outs[3][half:, :] = packed[...]
    for j, bit in enumerate(bits):
        set_bit = jnp.where((place[1] & bit) == 0, 0, 1)
        columns = slice(j * size, (j + 1) * size)
        to = slice((j % 2) * size, (j % 2 + 1) * size)
        outs[2 * (j // 2)][:half, to] = full[block(set_bit, half), columns]
        outs[2 * (j // 2) + 1][:half, to] = full[block(1 - set_bit, half), columns]
    outs[2][:half, size:] = out_keep[...]
    outs[3][:half, size:] = out_send[...]


def halve_kernel(bit, extra, place, kept, got, keep, send):
    set_bit = jnp.where((place[1] & bit) == 0, 0, 1)
    half = keep.shape[0] - extra
    for index, out in ((1 - set_bit, send), (set_bit, keep)):
        here = block(index, half)
        out[:half, :] = (kept[here, :].astype(F32) + got[here, :].astype(F32)).astype(BF)
        if extra:
            out[half:, :] = (kept[2 * half :, :].astype(F32) + got[2 * half :, :].astype(F32)).astype(BF)


def add_kernel(place, kept, got, out, *rest):
    half = out.shape[0]
    out[...] = (kept[:half, :].astype(F32) + got[:half, :].astype(F32)).astype(BF)
    for ref in rest:
        ref[...] = kept[half:, :].astype(F32) + got[half:, :].astype(F32)


def join_kernel(bit, place, mine, got, out):
    set_bit = jnp.where((place[1] & bit) == 0, 0, 1)
    half = mine.shape[0]
    for index, ref in ((set_bit, mine), (1 - set_bit, got)):
        out[block(index, half), :] = ref[...].astype(out.dtype)


def split_kernel(unstack):
    def shapes(height, width):
        return [((height, width // 2), F32), (unstack or (height, width // 2), F32)]

    def kernel(bit, place, mine, got, one, two):
        set_bit = jnp.where((place[1] & bit) == 0, 0, 1)
        half = mine.shape[0]
        size = one.shape[1]
        for index, ref in ((set_bit, mine), (1 - set_bit, got)):
            one[block(index, half), :] = ref[:, :size].astype(F32)
            if unstack:
                tall = unstack[0]
                for j in range(half // tall):
                    columns = block(index * (half // tall) + j, size)
                    two[:, columns] = ref[j * tall : (j + 1) * tall, size:].astype(F32)
            else:
                two[block(index, half), :] = ref[:, size:].astype(F32)

    return shapes, kernel


def whole_shapes(height, width):
    return [((height, width), F32)]


def dp_sum(line, keep, send, bits, name, last=(whole_shapes, join_kernel), extra=0):
    got = swap(send, "dp", bits[0])
    yield
    half, width = keep.shape
    half -= extra
    for bit in bits[1:]:
        half //= 2
        keep, send = line(
            functools.partial(halve_kernel, bit, extra),
            name + "_halve",
            [((half + extra, width), BF)] * 2,
            [keep, got],
        )
        got = swap(send, "dp", bit)
        yield
    mine, *rest = line(
        add_kernel, name + "_add", [((half, width), BF)] + [((extra, width), F32)] * (extra > 0), [keep, got]
    )
    got = swap(mine, "dp", bits[-1])
    yield
    for bit in reversed(bits[1:]):
        half *= 2
        (mine,) = line(
            functools.partial(join_kernel, bit), name + "_join", [((half, width), BF)], [mine, got]
        )
        got = swap(mine, "dp", bits[bits.index(bit) - 1])
        yield
    shapes, kernel = last
    whole = line(
        functools.partial(kernel, bits[0]), name + "_whole", shapes(2 * half, width), [mine, got]
    )
    return [*whole, *rest]


class Steps:
    def __init__(self, generator):
        self.generator = generator
        self.result = None
        self.go()

    def go(self, times=1):
        for _ in range(times):
            if self.result is None:
                try:
                    next(self.generator)
                except StopIteration as stop:
                    self.result = stop.value

    def finish(self):
        while self.result is None:
            self.go()
        return self.result


def small_pack_kernel(count, place, *refs):
    out = refs[-1]
    width = out.shape[1] // 2
    b_in = total_of([ref[...] for ref in refs[4 : 4 + 2 * count]])
    b_proj = total_of([ref[...] for ref in refs[4 + 2 * count : 4 + 3 * count]])
    features = total_of([ref[...] for ref in refs[:4]])
    rows = [features[i : i + 1, :] for i in range(6)]
    for whole in (b_in, b_proj):
        rows += [whole[:, j * width : (j + 1) * width] for j in range(whole.shape[1] // width)]
    rows += [jnp.zeros((1, width), F32)] * (2 * out.shape[0] - len(rows))
    left, right = jnp.concatenate(rows[0::2], axis=0), jnp.concatenate(rows[1::2], axis=0)
    out[...] = jnp.concatenate([left, right], axis=1).astype(BF)


def small_out_kernel(place, total, *outs):
    width = total.shape[1] // 2
    row = 0
    for out in outs:
        for j in range(out.shape[0] // width):
            out[j * width : (j + 1) * width] = total[row // 2, (row % 2) * width : (row % 2 + 1) * width]
            row += 1


def out_pack_kernel(count, place, *refs):
    t = place[0]
    r = refs[0].shape[0]
    for k, out in enumerate(refs[count:]):
        for i in range(count):
            out[i * r : (i + 1) * r, :] = refs[i][:, block(t ^ k, out.shape[1])]


def rows_kernel(count, place, *refs):
    t = place[0]
    out = refs[-1]
    r = refs[0].shape[0] // count
    for k in range(4):
        for i in range(count):
            out[block(4 * i + (t ^ k), r), :] = refs[k][i * r : (i + 1) * r, :]


def tokens_kernel(place, *refs):
    out = refs[-1]
    r = refs[0].shape[0]
    for i in range((len(refs) - 1) // 4):
        terms = [first_of(refs[4 * i + j]) for j in range(4)]
        out[i * r : (i + 1) * r, :] = total_of(terms).astype(BF)


def pack_kernel(count, place, *refs):
    t = place[0]
    outs, spread = refs[2 * count : 2 * count + 4], refs[-1]
    spread[0:3, :] = total_of([refs[i][...] for i in range(count)])
    spread[3:6, :] = total_of([refs[count + i][...] for i in range(count)])
    width = outs[0].shape[1]
    for k, ref in enumerate(outs):
        ref[...] = spread[0:6, block(t ^ k, width)]


def total_of(parts):
    return functools.reduce(lambda a, b: a + b, parts)


def local(
    tokens,
    segment_ids,
    w_query,
    w_key,
    w_value,
    b_query,
    b_value,
    w_out,
    b_out,
    gain_one,
    bias_one,
    w_in,
    b_in,
    w_down,
    b_down,
    gain_two,
    bias_two,
    cotangent,
):
    t = lax.axis_index("tensor")
    d = lax.axis_index("dp")
    line = Line(jnp.stack([t, d]).astype(jnp.int32))
    row_count, cols = tokens.shape
    width = w_query.shape[0]
    units = w_in.shape[1]
    count = row_count // LEN
    r = LEN // 4
    heads = cols // HD
    labels = segment_ids.reshape(count, 1, LEN)
    every = range(count)
    spread = pltpu.VMEM((8, width), F32)

    first, rest = tokens[:LEN], tokens[LEN:]
    rest_across = swap(rest, "tensor", 2)
    pieces = [gather_blocks(first)]

    def onward(kept, got, pair):
        (both,) = line(
            second_of_onward_kernel if pair else onward_kernel,
            "onward",
            [(kept.shape[1:] if pair else kept.shape, BF)],
            [kept, got],
        )
        return swap(both, "tensor", 2)

    ctxs, projs, totals, attn_terms = [], [], [], []

    def do_attend(i):
        proj, ctx, total, residual, keep, send = line(
            functools.partial(attend_kernel, max(i - 1, 0)),
            "attend",
            [
                ((LEN, 3 * cols), BF),
                ((LEN, cols), BF),
                ((LEN, heads), F32),
                ((r, width), BF),
                ((2, r, width), BF),
                ((2, r, width), BF),
            ],
            [*pieces[min(i, 1)], w_query, w_key, w_value, b_query, b_value, labels[i], w_out],
            flops=2 * LEN * width * 4 * cols + 4 * LEN * LEN * cols * heads,
            exps=heads * LEN * LEN,
        )
        attn_terms.append((keep, swap(send, "tensor", 1), residual))
        projs.append(proj)
        ctxs.append(ctx)
        totals.append(total)

    def do_attend_onward(i):
        keep, sent, residual = attn_terms[i]
        attn_terms[i] = [keep, sent, onward(keep, sent, True), residual]

    firsts, h_pieces = [], []

    def do_first_norm(i):
        normed, inverse, low = line(
            first_norm_kernel,
            "first_norm",
            [((r, width), F32), ((r, 1), F32), ((r, width), BF)],
            [*attn_terms[i], *vectors],
            flops=20 * r * width,
            scratch=[spread],
        )
        firsts.append((normed, inverse))
        h_pieces.append(gather_blocks(low))

    feeds = {}

    def do_feed(i, j):
        feeds[i, j] = line(
            feed_kernel,
            "feed",
            [((2 * r, units), BF), ((2 * r, units), BF), ((r, width), BF), ((r, width), BF)],
            [*h_pieces[i][2 * j : 2 * j + 2], w_in, b_in, w_down],
            flops=8 * r * width * units,
            exps=2 * r * units * 2,
        )

    seconds, dz_pieces, results = [], [], []

    def do_second_norm(i):
        dz, low, result, sums = line(
            functools.partial(second_norm_kernel, i),
            "second_norm",
            [((r, width), F32), ((r, width), BF), ((r, width), BF), ((3, width), F32)],
            [
                *feed_terms[i],
                firsts[i][0],
                *cots,
                *vectors,
            ],
            flops=40 * r * width,
            scratch=[spread, pltpu.VMEM((r, width), F32)],
        )
        seconds.append((dz, sums))
        results.append(result)
        dz_pieces.append(gather_blocks(low))

    backs = {}

    def do_feed_back(i, j):
        backs[i, j] = line(
            feed_back_kernel,
            "feed_back",
            [((2 * r, units), BF), ((r, width), BF), ((r, width), BF), ((1, units), F32)],
            [*dz_pieces[i][2 * j : 2 * j + 2], feeds[i, j][1], w_down, w_in],
            flops=8 * r * width * units,
        )

    thirds, dz1_pieces = [], []

    def do_first_back(i):
        low, sums = line(
            first_back_kernel,
            "first_back",
            [((r, width), BF), ((3, width), F32)],
            [*back_terms[i], seconds[i][0], *firsts[i], *vectors],
            flops=30 * r * width,
            scratch=[spread],
        )
        thirds.append(sums)
        dz1_pieces.append(gather_blocks(low))

    dprojs, token_terms, b_proj_parts = [], [], []

    def do_attend_back(i):
        dproj, keep, send, dz_cols, bias = line(
            attend_back_kernel,
            "attend_back",
            [
                ((LEN, 3 * cols), BF),
                ((2, LEN, cols), BF),
                ((2, LEN, cols), BF),
                ((LEN, cols), BF),
                ((1, 3 * cols), F32),
            ],
            [*dz1_pieces[i], w_out, projs[i], totals[i], labels[i], w_query, w_key, w_value],
            flops=2 * LEN * width * 4 * cols + 10 * LEN * LEN * cols * heads,
            exps=heads * LEN * LEN,
            scratch=[pltpu.VMEM((LEN, cols), BF)],
        )
        token_terms.append((dz_cols, keep, swap(send, "tensor", 1)))
        dprojs.append(dproj)
        b_proj_parts.append(bias)

    def do_tokens_onward(i):
        dz_cols, keep, sent = token_terms[i]
        token_terms[i] = [dz_cols, keep, sent, onward(keep, sent, True)]

    feed_terms, back_terms = {}, {}

    def send_beside(terms, i, b0, b1, b2, b3):
        terms[i] = (b0, swap(b1, "tensor", 1), b2, swap(b3, "tensor", 1))

    def send_across(terms, i):
        b0, near, b2, far = terms[i]
        terms[i] = (b0, near, onward(b2, far, False))

    def staggered(first, second):
        for i in every:
            first(i)
            if i:
                second(i - 1)

    do_attend(0)
    (vectors,) = line(
        vectors_kernel, "vectors", [((6, cols), BF)], [b_out, gain_one, bias_one, b_down, gain_two, bias_two]
    )
    vectors = gather_blocks(vectors)
    cots = exchange_blocks(
        line(
            functools.partial(cot_pack_kernel, count), "cot_pack", [((count * r, cols), BF)] * 4, [cotangent]
        )
    )
    rest_across = line.after(rest_across)
    pieces.append((rest, swap(rest, "tensor", 1), rest_across, swap(rest_across, "tensor", 1)))
    for i in every[1:]:
        do_attend(i)
        do_attend_onward(i - 1)
        if i == 1:
            line.take(*cots)
    do_attend_onward(count - 1)

    for i in every:
        do_first_norm(i)
        do_feed(i, 0)

    def second_feed(i):
        do_feed(i, 1)
        send_beside(feed_terms, i, *feeds[i, 0][2:], *feeds[i, 1][2:])

    staggered(second_feed, lambda i: send_across(feed_terms, i))
    send_across(feed_terms, count - 1)
    for i in every:
        do_second_norm(i)
        do_feed_back(i, 0)

    early, late = dp_bits(0), dp_bits(1)

    def second_back(i):
        do_feed_back(i, 1)
        send_beside(back_terms, i, *backs[i, 0][1:3], *backs[i, 1][1:3])

    for i in every[:-1]:
        second_back(i)
        if i:
            send_across(back_terms, i - 1)
    down_pairs = [
        ([feeds[i, j][0]], dz_pieces[i][2 * j : 2 * j + 2]) for i in every for j in range(2)
    ]
    down = Steps(
        dp_sum(line, *weight_grad(line, down_pairs, units, width, early[0], "down_grad"), early, "down")
    )
    for i in every[-2:-1]:
        send_across(back_terms, i)
    second_back(count - 1)
    in_pairs = [
        (h_pieces[i][2 * j : 2 * j + 2], [backs[i, j][0]]) for i in every for j in range(2)
    ]
    into = Steps(
        dp_sum(line, *weight_grad(line, in_pairs, width, units, early[0], "in_grad"), early, "into")
    )
    send_across(back_terms, count - 1)
    for i in every[:-1]:
        do_first_back(i)
    down.go()
    do_first_back(count - 1)
    pieces_out = exchange_blocks(
        line(
            functools.partial(out_pack_kernel, count),
            "out_pack",
            [((count * r, cols), BF)] * 4,
            results,
        )
    )
    wide = exchange_blocks(
        line(
            functools.partial(pack_kernel, count),
            "pack",
            [((6, cols), F32)] * 4,
            [s for _, s in seconds] + thirds,
            scratch=[spread],
        )
    )

    do_attend_back(0)
    down.go()
    into.go()
    do_attend_back(1 % count)
    for i in every[2:]:
        do_attend_back(i)
    down.go()
    into.go()
    out_pairs = [([ctxs[i]], [dz1_pieces[i][k] for k in range(4)]) for i in every]
    out_half = weight_grad(line, out_pairs, width, cols, late[0], "out_grad", stacked=True)
    extra = -(-(6 + units // cols + 3) // 32) * 16
    (packed,) = line(
        functools.partial(small_pack_kernel, count),
        "small_pack",
        [((extra, 2 * cols), BF)],
        [*wide, *[b[3] for b in backs.values()], *b_proj_parts],
    )
    half_shape = ((width // 2, 2 * cols), BF)
    more_shape = ((width // 2 + extra, 2 * cols), BF)
    first_half = line(
        functools.partial(proj_grad_kernel, count, (early[0], early[0], late[0])),
        "proj_grad",
        [half_shape, half_shape, more_shape, more_shape],
        [*pieces[0], *pieces[1], *dprojs, *out_half, packed],
        flops=2 * row_count * width * 3 * cols,
        scratch=[pltpu.VMEM((width, 3 * cols), BF)],
    )
    query_key = Steps(dp_sum(line, first_half[0], first_half[1], early, "query_key", split_kernel(None)))
    value_out = Steps(
        dp_sum(line, first_half[2], first_half[3], late, "value_out", split_kernel((cols, width)), extra)
    )
    down.go()
    into.go()
    for i in every:
        do_tokens_onward(i)
    query_key.go()
    value_out.go()
    down.go()
    into.go()
    query_key.go()
    value_out.go()
    into.go()
    (result,) = line(
        functools.partial(rows_kernel, count), "out_rows", [((row_count, cols), BF)], pieces_out
    )
    query_key.go()
    value_out.go()
    (grad_tokens,) = line(
        tokens_kernel, "token_rows", [((row_count, cols), BF)], [x for terms in token_terms for x in terms]
    )
    query_key.go()
    value_out.go()
    down.go()
    query_key.go()
    value_out.go()
    into.go()
    query_key.go()
    value_out.go()
    waiting = [query_key, value_out, into, down]
    while any(s.result is None for s in waiting):
        for s in waiting:
            s.go()
    sums = line(
        small_out_kernel,
        "small_out",
        [((s,), F32) for s in [cols] * 6 + [units] + [cols] * 3],
        [value_out.result[2]],
    )

    return (
        result,
        grad_tokens,
        query_key.result[0],
        query_key.result[1],
        value_out.result[0],
        sums[7],
        sums[9],
        value_out.result[1],
        sums[5],
        sums[3],
        sums[4],
        into.result[0],
        sums[6],
        down.result[0],
        sums[2],
        sums[0],
        sums[1],
    )


def solution(mesh):
    placed = (
        P("dp", "tensor"),
        P("dp"),
        P(None, "tensor"),
        P(None, "tensor"),
        P(None, "tensor"),
        P("tensor"),
        P("tensor"),
        P("tensor", None),
        P("tensor"),
        P("tensor"),
        P("tensor"),
        P(None, "tensor"),
        P("tensor"),
        P("tensor", None),
        P("tensor"),
        P("tensor"),
        P("tensor"),
        P("dp", "tensor"),
    )
    return jax.shard_map(
        local,
        mesh=mesh,
        in_specs=placed,
        out_specs=(
            P("dp", "tensor"),
            P("dp", "tensor"),
            P(None, "tensor"),
            P(None, "tensor"),
            P(None, "tensor"),
            P("tensor"),
            P("tensor"),
            P("tensor", None),
            P("tensor"),
            P("tensor"),
            P("tensor"),
            P(None, "tensor"),
            P("tensor"),
            P("tensor", None),
            P("tensor"),
            P("tensor"),
            P("tensor"),
        ),
        check_vma=False,
    )
```

```python
import functools
import math

import jax
import jax.numpy as jnp
from jax import lax
from jax.experimental import pallas as pl
from jax.experimental.pallas import tpu as pltpu
from jax.sharding import PartitionSpec as P

HD = 64
LEN = 512

EPSILON = 1e-05
MASKED = -1000000000.0
VMEM_LIMIT = 8 << 20
BF = jnp.bfloat16
F32 = jnp.float32


def mm(left, right):
    return lax.dot_general(left, right, (((1,), (0,)), ((), ())), preferred_element_type=F32)


def over_rows(left, right):
    return lax.dot_general(left, right, (((0,), (0,)), ((), ())), preferred_element_type=F32)


def against(left, right):
    return lax.dot_general(left, right, (((1,), (1,)), ((), ())), preferred_element_type=F32)


def swap(values, axis, bit):
    size = lax.axis_size(axis)
    return lax.ppermute(values, axis, [(i, i ^ bit) for i in range(size)])


def gather_blocks(own):
    across = swap(own, "tensor", 2)
    beside = swap(own, "tensor", 1)
    corner = swap(across, "tensor", 1)
    return own, beside, across, corner


def exchange_blocks(blocks):
    return (
        blocks[0],
        swap(blocks[1], "tensor", 1),
        swap(blocks[2], "tensor", 2),
        swap(blocks[3], "tensor", 3),
    )


def dp_bits(order):
    size = lax.axis_size("dp")
    bits = [1 << i for i in range(int(math.log2(size)))]
    if order and len(bits) > 1:
        bits[0], bits[1] = bits[1], bits[0]
    return bits


class Line:
    def __init__(self, place):
        self.place = place

    def __call__(self, kernel, name, out_shape, operands, flops=0, exps=0, scratch=()):
        out_shape = [jax.ShapeDtypeStruct(s, d) for s, d in out_shape]
        size = sum(math.prod(o.shape) * o.dtype.itemsize for o in list(operands) + out_shape)
        whole = pl.BlockSpec(memory_space=pltpu.VMEM)
        outs = pl.pallas_call(
            kernel,
            in_specs=[pl.BlockSpec(memory_space=pltpu.SMEM)] + [whole] * len(operands),
            out_specs=[whole] * len(out_shape),
            out_shape=out_shape,
            scratch_shapes=list(scratch),
            compiler_params=pltpu.CompilerParams(vmem_limit_bytes=VMEM_LIMIT),
            cost_estimate=pl.CostEstimate(flops=flops, transcendentals=exps, bytes_accessed=size),
            name=name,
        )(self.place, *operands)
        last = min(outs, key=lambda o: math.prod(o.shape))
        self.place, _ = lax.optimization_barrier((self.place, last))
        return outs

    def after(self, value):
        return lax.optimization_barrier((value, self.place))[0]

    def take(self, *values):
        self.place = lax.optimization_barrier((self.place, *values))[0]


def block(index, size):
    return pl.ds(pl.multiple_of(index * size, size), size)


def first_of(ref):
    return (ref[0] if len(ref.shape) == 3 else ref[...]).astype(F32)


def head_lanes(width, head):
    lane = lax.broadcasted_iota(jnp.int32, (1, width), 1)
    return (lane >= head * HD) & (lane < (head + 1) * HD)


def allowed_block(label_row):
    length = label_row.shape[1]
    label_row = label_row.astype(F32)
    label_column = jnp.transpose(jnp.broadcast_to(label_row, (8, length)))[:, :1]
    same = label_column == label_row
    diagonal = lax.broadcasted_iota(jnp.int32, (length, length), 0) == lax.broadcasted_iota(
        jnp.int32, (length, length), 1
    )
    return same & ((label_column != 0.0) | diagonal)


def attend_kernel(
    sequence, place, p0, p1, p2, p3, wq, wk, wv, bq, bv, label, w_out, proj, ctx, total, residual, keep, send
):
    t = place[0]
    width = wq.shape[1]
    length = ctx.shape[0]
    rows = length // 4
    pieces = [p.at[sequence * length : (sequence + 1) * length, :] for p in (p0, p1, p2, p3)]
    for k, piece in enumerate(pieces):
        residual[:, block(t ^ k, width)] = piece[block(t, rows), :]
    parts = []
    for weight in (wq, wk, wv):
        parts.append(total_of([mm(piece[...], weight[block(t ^ k, width), :]) for k, piece in enumerate(pieces)]))
    queries = (parts[0] + bq[...].astype(F32)[None, :]).astype(BF)
    keys = parts[1].astype(BF)
    values = (parts[2] + bv[...].astype(F32)[None, :]).astype(BF)
    proj[:, :width] = queries
    proj[:, width : 2 * width] = keys
    proj[:, 2 * width :] = values
    allowed = allowed_block(label[...])
    context = jnp.zeros(queries.shape, F32)
    zero = jnp.zeros((), BF)
    for head in range(width // HD):
        lanes = head_lanes(width, head)
        scores = against(jnp.where(lanes, queries, zero), keys) * (HD**-0.5)
        scores = jnp.where(allowed, scores, MASKED)
        peak = jnp.max(scores, axis=1, keepdims=True)
        terms = jnp.exp(scores - peak)
        summed = jnp.sum(terms, axis=1, keepdims=True)
        probs = (terms / summed).astype(BF)
        context = context + mm(probs, jnp.where(lanes, values, zero))
        total[:, head : head + 1] = peak + jnp.log(summed)
    context = context.astype(BF)
    for j in range(4):
        ctx[block(t ^ j, rows), :] = context[j * rows : (j + 1) * rows]
    for k in range(4):
        part = mm(ctx[k * rows : (k + 1) * rows, :], w_out[...]).astype(BF)
        (send if k % 2 else keep)[k // 2] = part


def attend_back_kernel(
    place, d0, d1, d2, d3, w_out, proj, total, label, wq, wk, wv, dproj, keep, send, dz_cols, bias, dctx
):
    t = place[0]
    width = wq.shape[1]
    rows = d0.shape[0]
    for k, piece in enumerate((d0, d1, d2, d3)):
        dctx[block(t ^ k, rows), :] = against(piece[...], w_out[...]).astype(BF)
        dz_cols[block(t ^ k, rows), :] = piece[:, block(t, width)]
    allowed = allowed_block(label[...])
    queries, keys, values = proj[:, :width], proj[:, width : 2 * width], proj[:, 2 * width :]
    dcontext = dctx[...]
    scale = HD**-0.5
    dquery = jnp.zeros(queries.shape, F32)
    dkey = jnp.zeros(queries.shape, F32)
    dvalue = jnp.zeros(queries.shape, F32)
    zero = jnp.zeros((), BF)
    for head in range(width // HD):
        lanes = head_lanes(width, head)
        q_head = jnp.where(lanes, queries, zero)
        d_head = jnp.where(lanes, dcontext, zero)
        k_head = jnp.where(lanes, keys, zero)
        scores = against(q_head, keys) * scale
        scores = jnp.where(allowed, scores, MASKED)
        probs = jnp.exp(scores - total[:, head : head + 1])
        dprobs = against(d_head, values)
        delta = jnp.sum(probs * dprobs, axis=1, keepdims=True)
        dscores = (probs * (dprobs - delta)).astype(BF)
        dquery = dquery + mm(dscores, k_head)
        dkey = dkey + over_rows(dscores, q_head)
        dvalue = dvalue + over_rows(probs.astype(BF), d_head)
    grads = ((dquery * scale).astype(BF), (dkey * scale).astype(BF), dvalue.astype(BF))
    for i, grad in enumerate(grads):
        dproj[:, i * width : (i + 1) * width] = grad
        bias[:, i * width : (i + 1) * width] = jnp.sum(grad.astype(F32), axis=0, keepdims=True)
    for k in range(4):
        here = block(t ^ k, width)
        part = total_of([against(grad, weight[here, :]) for grad, weight in zip(grads, (wq, wk, wv))])
        (send if k % 2 else keep)[k // 2] = part.astype(BF)


def normed_of(values):
    center = values - jnp.mean(values, axis=1, keepdims=True)
    inverse = lax.rsqrt(jnp.mean(center * center, axis=1, keepdims=True) + EPSILON)
    return center * inverse, inverse


def norm_back(scaled, normed, inverse):
    mean = jnp.mean(scaled, axis=1, keepdims=True)
    along = jnp.mean(scaled * normed, axis=1, keepdims=True)
    return inverse * (scaled - mean - normed * along)


def fill(vectors, spread, t):
    width = vectors[0].shape[1]
    for k, ref in enumerate(vectors):
        spread[0:6, block(t ^ k, width)] = ref[...].astype(F32)


def onward_kernel(place, kept, got, out):
    out[...] = (kept[...].astype(F32) + got[...].astype(F32)).astype(BF)


def second_of_onward_kernel(place, kept, got, out):
    out[...] = (kept[1].astype(F32) + got[1].astype(F32)).astype(BF)


def vectors_kernel(place, *refs):
    for i, ref in enumerate(refs[:-1]):
        refs[-1][i : i + 1, :] = ref[...][None, :]


def first_norm_kernel(place, s0, s1, s2, residual, v0, v1, v2, v3, normed_ref, inverse_ref, low, spread):
    fill((v0, v1, v2, v3), spread, place[0])
    z = first_of(s0) + first_of(s1) + first_of(s2)
    z = residual[...].astype(F32) + z + spread[0:1, :]
    normed, inverse = normed_of(z)
    normed_ref[...] = normed
    inverse_ref[...] = inverse
    low[...] = (normed * spread[1:2, :] + spread[2:3, :]).astype(BF)


def cot_pack_kernel(count, place, cot, *outs):
    t = place[0]
    r = outs[0].shape[0] // count
    for k, out in enumerate(outs):
        for i in range(count):
            out[i * r : (i + 1) * r, :] = cot[block(4 * i + (t ^ k), r), :]


def second_norm_kernel(
    sequence, place, s0, s1, s2, normed_one, c0, c1, c2, c3, v0, v1, v2, v3, dz, low, out, sums, spread, cots
):
    t = place[0]
    fill((v0, v1, v2, v3), spread, t)
    width = c0.shape[1]
    r = dz.shape[0]
    for k, ref in enumerate((c0, c1, c2, c3)):
        cots[:, block(t ^ k, width)] = ref[sequence * r : (sequence + 1) * r, :].astype(F32)
    h_one = normed_one[...] * spread[1:2, :] + spread[2:3, :]
    z = h_one + (s0[...].astype(F32) + s1[...].astype(F32) + s2[...].astype(F32)) + spread[3:4, :]
    normed, inverse = normed_of(z)
    out[...] = (normed * spread[4:5, :] + spread[5:6, :]).astype(BF)
    grad = cots[...]
    sums[0:1, :] = jnp.sum(grad * normed, axis=0, keepdims=True)
    sums[1:2, :] = jnp.sum(grad, axis=0, keepdims=True)
    back = norm_back(grad * spread[4:5, :], normed, inverse)
    sums[2:3, :] = jnp.sum(back, axis=0, keepdims=True)
    dz[...] = back
    low[...] = back.astype(BF)


def first_back_kernel(place, s0, s1, s2, dz, normed_ref, inverse_ref, v0, v1, v2, v3, low, sums, spread):
    fill((v0, v1, v2, v3), spread, place[0])
    dh = dz[...] + (s0[...].astype(F32) + s1[...].astype(F32) + s2[...].astype(F32))
    normed = normed_ref[...]
    sums[0:1, :] = jnp.sum(dh * normed, axis=0, keepdims=True)
    sums[1:2, :] = jnp.sum(dh, axis=0, keepdims=True)
    back = norm_back(dh * spread[1:2, :], normed, inverse_ref[...])
    sums[2:3, :] = jnp.sum(back, axis=0, keepdims=True)
    low[...] = back.astype(BF)


def feed_kernel(place, h0, h1, w_in, b_in, w_down, hidden, slope, keep, send):
    rows = jnp.concatenate([h0[...], h1[...]], axis=0)
    r = h0.shape[0]
    units = w_in.shape[1]
    step = min(256, units)
    total = jnp.zeros((2 * r, w_down.shape[1]), F32)
    for first in range(0, units, step):
        here = slice(first, first + step)
        pre_act = mm(rows, w_in[:, here]) + b_in[here].astype(F32)[None, :]
        cdf = 0.5 * (1.0 + lax.erf(pre_act * (2.0**-0.5)))
        rise = pre_act * jnp.exp(-0.5 * pre_act * pre_act) * ((2.0 * math.pi) ** -0.5)
        active = (pre_act * cdf).astype(BF)
        hidden[:, here] = active
        slope[:, here] = (cdf + rise).astype(BF)
        total = total + mm(active, w_down[here, :])
    keep[...] = total[:r].astype(BF)
    send[...] = total[r:].astype(BF)


def feed_back_kernel(place, d0, d1, slope, w_down, w_in, dpre, keep, send, bias):
    rows = jnp.concatenate([d0[...], d1[...]], axis=0)
    r = d0.shape[0]
    units = w_in.shape[1]
    step = min(256, units)
    total = jnp.zeros((2 * r, w_in.shape[0]), F32)
    for first in range(0, units, step):
        here = slice(first, first + step)
        grad = (against(rows, w_down[here, :]) * slope[:, here].astype(F32)).astype(BF)
        dpre[:, here] = grad
        bias[:, here] = jnp.sum(grad.astype(F32), axis=0, keepdims=True)
        total = total + against(grad, w_in[:, here])
    keep[...] = total[:r].astype(BF)
    send[...] = total[r:].astype(BF)


def weight_grad_kernel(groups, stacked, bit, place, *refs):
    keep, send = refs[-2:]
    set_bit = jnp.where((place[1] & bit) == 0, 0, 1)
    lefts, rights = [], []
    at = 0
    for left, right in groups:
        lefts.append(refs[at : at + left])
        rights.append(refs[at + left : at + left + right])
        at += left + right

    def joined(parts, columns):
        parts = [p[:, columns] for p in parts]
        return parts[0] if len(parts) == 1 else jnp.concatenate(parts, axis=0)

    half, width = keep.shape
    step = min(256, half)
    for half_index, out in ((1 - set_bit, send), (set_bit, keep)):
        for first in range(0, half, step):
            here = block(half_index * (half // step) + first // step, step)
            if stacked:
                terms = [over_rows(joined(l, slice(None)), joined(r, here)) for l, r in zip(lefts, rights)]
            else:
                terms = [over_rows(joined(l, here), joined(r, slice(None))) for l, r in zip(lefts, rights)]
            out[first : first + step, :] = total_of(terms).astype(BF)


def weight_grad(line, pairs, height, width, bit, name, stacked=False):
    operands = [x for left, right in pairs for x in (*left, *right)]
    groups = [(len(left), len(right)) for left, right in pairs]
    depth = sum(x.shape[0] for left, _ in pairs for x in left)
    return line(
        functools.partial(weight_grad_kernel, groups, stacked, bit),
        name,
        [((height // 2, width), BF)] * 2,
        operands,
        flops=2 * depth * height * width,
    )


def proj_grad_kernel(count, bits, place, *refs):
    t = place[0]
    out_keep, out_send, packed = refs[8 + count : 11 + count]
    outs, full = refs[-5:-1], refs[-1]
    size = refs[0].shape[1]
    rows = refs[0].shape[0]
    for k in range(4):
        terms = [over_rows(refs[k][...], refs[8][...])]
        for i in range(1, count):
            terms.append(over_rows(refs[4 + k][(i - 1) * rows : i * rows, :], refs[8 + i][...]))
        full[block(t ^ k, size), :] = total_of(terms).astype(BF)
    half = outs[0].shape[0]
    outs[2][half:, :] = packed[...]
    outs[3][half:, :] = packed[...]
    for j, bit in enumerate(bits):
        set_bit = jnp.where((place[1] & bit) == 0, 0, 1)
        columns = slice(j * size, (j + 1) * size)
        to = slice((j % 2) * size, (j % 2 + 1) * size)
        outs[2 * (j // 2)][:half, to] = full[block(set_bit, half), columns]
        outs[2 * (j // 2) + 1][:half, to] = full[block(1 - set_bit, half), columns]
    outs[2][:half, size:] = out_keep[...]
    outs[3][:half, size:] = out_send[...]


def halve_kernel(bit, extra, place, kept, got, keep, send):
    set_bit = jnp.where((place[1] & bit) == 0, 0, 1)
    half = keep.shape[0] - extra
    for index, out in ((1 - set_bit, send), (set_bit, keep)):
        here = block(index, half)
        out[:half, :] = (kept[here, :].astype(F32) + got[here, :].astype(F32)).astype(BF)
        if extra:
            out[half:, :] = (kept[2 * half :, :].astype(F32) + got[2 * half :, :].astype(F32)).astype(BF)


def add_kernel(place, kept, got, out, *rest):
    half = out.shape[0]
    out[...] = (kept[:half, :].astype(F32) + got[:half, :].astype(F32)).astype(BF)
    for ref in rest:
        ref[...] = kept[half:, :].astype(F32) + got[half:, :].astype(F32)


def join_kernel(bit, place, mine, got, out):
    set_bit = jnp.where((place[1] & bit) == 0, 0, 1)
    half = mine.shape[0]
    for index, ref in ((set_bit, mine), (1 - set_bit, got)):
        out[block(index, half), :] = ref[...].astype(out.dtype)


def split_kernel(unstack):
    def shapes(height, width):
        return [((height, width // 2), F32), (unstack or (height, width // 2), F32)]

    def kernel(bit, place, mine, got, one, two):
        set_bit = jnp.where((place[1] & bit) == 0, 0, 1)
        half = mine.shape[0]
        size = one.shape[1]
        for index, ref in ((set_bit, mine), (1 - set_bit, got)):
            one[block(index, half), :] = ref[:, :size].astype(F32)
            if unstack:
                tall = unstack[0]
                for j in range(half // tall):
                    columns = block(index * (half // tall) + j, size)
                    two[:, columns] = ref[j * tall : (j + 1) * tall, size:].astype(F32)
            else:
                two[block(index, half), :] = ref[:, size:].astype(F32)

    return shapes, kernel


def whole_shapes(height, width):
    return [((height, width), F32)]


def dp_sum(line, keep, send, bits, name, last=(whole_shapes, join_kernel), extra=0, rests=()):
    got = swap(send, "dp", bits[0])
    yield
    half, width = keep.shape
    half -= extra
    for bit in bits[1:]:
        half //= 2
        keep, send = line(
            functools.partial(halve_kernel, bit, extra),
            name + "_halve",
            [((half + extra, width), BF)] * 2,
            [keep, got],
        )
        got = swap(send, "dp", bit)
        yield
    mine, *rest = line(
        add_kernel, name + "_add", [((half, width), BF)] + [((extra, width), F32)] * (extra > 0), [keep, got]
    )
    if extra:
        rests.extend(rest)
    got = swap(mine, "dp", bits[-1])
    yield
    for bit in reversed(bits[1:]):
        half *= 2
        (mine,) = line(
            functools.partial(join_kernel, bit), name + "_join", [((half, width), BF)], [mine, got]
        )
        got = swap(mine, "dp", bits[bits.index(bit) - 1])
        yield
    shapes, kernel = last
    return line(
        functools.partial(kernel, bits[0]), name + "_whole", shapes(2 * half, width), [mine, got]
    )


class Steps:
    def __init__(self, generator):
        self.generator = generator
        self.result = None
        self.go()

    def go(self, times=1):
        for _ in range(times):
            if self.result is None:
                try:
                    next(self.generator)
                except StopIteration as stop:
                    self.result = stop.value

    def finish(self):
        while self.result is None:
            self.go()
        return self.result


def small_pack_kernel(count, place, *refs):
    out = refs[-1]
    width = out.shape[1] // 2
    b_in = total_of([ref[...] for ref in refs[4 : 4 + 2 * count]])
    b_proj = total_of([ref[...] for ref in refs[4 + 2 * count : 4 + 3 * count]])
    features = total_of([ref[...] for ref in refs[:4]])
    rows = [features[i : i + 1, :] for i in range(6)]
    for whole in (b_in, b_proj):
        rows += [whole[:, j * width : (j + 1) * width] for j in range(whole.shape[1] // width)]
    rows += [jnp.zeros((1, width), F32)] * (2 * out.shape[0] - len(rows))
    left, right = jnp.concatenate(rows[0::2], axis=0), jnp.concatenate(rows[1::2], axis=0)
    out[...] = jnp.concatenate([left, right], axis=1).astype(BF)


def small_out_kernel(place, total, *outs):
    width = total.shape[1] // 2
    row = 0
    for out in outs:
        for j in range(out.shape[0] // width):
            out[j * width : (j + 1) * width] = total[row // 2, (row % 2) * width : (row % 2 + 1) * width]
            row += 1


def out_pack_kernel(count, place, *refs):
    t = place[0]
    r = refs[0].shape[0]
    for k, out in enumerate(refs[count:]):
        for i in range(count):
            out[i * r : (i + 1) * r, :] = refs[i][:, block(t ^ k, out.shape[1])]


def rows_kernel(count, place, *refs):
    t = place[0]
    out = refs[-1]
    r = refs[0].shape[0] // count
    for k in range(4):
        for i in range(count):
            out[block(4 * i + (t ^ k), r), :] = refs[k][i * r : (i + 1) * r, :]


def tokens_kernel(place, *refs):
    out = refs[-1]
    r = refs[0].shape[0]
    for i in range((len(refs) - 1) // 4):
        terms = [first_of(refs[4 * i + j]) for j in range(4)]
        out[i * r : (i + 1) * r, :] = total_of(terms).astype(BF)


def pack_kernel(count, place, *refs):
    t = place[0]
    outs, spread = refs[2 * count : 2 * count + 4], refs[-1]
    spread[0:3, :] = total_of([refs[i][...] for i in range(count)])
    spread[3:6, :] = total_of([refs[count + i][...] for i in range(count)])
    width = outs[0].shape[1]
    for k, ref in enumerate(outs):
        ref[...] = spread[0:6, block(t ^ k, width)]


def total_of(parts):
    return functools.reduce(lambda a, b: a + b, parts)


def local(
    tokens,
    segment_ids,
    w_query,
    w_key,
    w_value,
    b_query,
    b_value,
    w_out,
    b_out,
    gain_one,
    bias_one,
    w_in,
    b_in,
    w_down,
    b_down,
    gain_two,
    bias_two,
    cotangent,
):
    t = lax.axis_index("tensor")
    d = lax.axis_index("dp")
    line = Line(jnp.stack([t, d]).astype(jnp.int32))
    row_count, cols = tokens.shape
    width = w_query.shape[0]
    units = w_in.shape[1]
    count = row_count // LEN
    r = LEN // 4
    heads = cols // HD
    labels = segment_ids.reshape(count, 1, LEN)
    every = range(count)
    spread = pltpu.VMEM((8, width), F32)

    first, rest = tokens[:LEN], tokens[LEN:]
    rest_across = swap(rest, "tensor", 2)
    pieces = [gather_blocks(first)]

    def onward(kept, got, pair):
        (both,) = line(
            second_of_onward_kernel if pair else onward_kernel,
            "onward",
            [(kept.shape[1:] if pair else kept.shape, BF)],
            [kept, got],
        )
        return swap(both, "tensor", 2)

    ctxs, projs, totals, attn_terms = [], [], [], []

    def do_attend(i):
        proj, ctx, total, residual, keep, send = line(
            functools.partial(attend_kernel, max(i - 1, 0)),
            "attend",
            [
                ((LEN, 3 * cols), BF),
                ((LEN, cols), BF),
                ((LEN, heads), F32),
                ((r, width), BF),
                ((2, r, width), BF),
                ((2, r, width), BF),
            ],
            [*pieces[min(i, 1)], w_query, w_key, w_value, b_query, b_value, labels[i], w_out],
            flops=2 * LEN * width * 4 * cols + 4 * LEN * LEN * cols * heads,
            exps=heads * LEN * LEN,
        )
        attn_terms.append((keep, swap(send, "tensor", 1), residual))
        projs.append(proj)
        ctxs.append(ctx)
        totals.append(total)

    def do_attend_onward(i):
        keep, sent, residual = attn_terms[i]
        attn_terms[i] = [keep, sent, onward(keep, sent, True), residual]

    firsts, h_pieces = [], []

    def do_first_norm(i):
        normed, inverse, low = line(
            first_norm_kernel,
            "first_norm",
            [((r, width), F32), ((r, 1), F32), ((r, width), BF)],
            [*attn_terms[i], *vectors],
            flops=20 * r * width,
            scratch=[spread],
        )
        firsts.append((normed, inverse))
        h_pieces.append(gather_blocks(low))

    feeds = {}

    def do_feed(i, j):
        feeds[i, j] = line(
            feed_kernel,
            "feed",
            [((2 * r, units), BF), ((2 * r, units), BF), ((r, width), BF), ((r, width), BF)],
            [*h_pieces[i][2 * j : 2 * j + 2], w_in, b_in, w_down],
            flops=8 * r * width * units,
            exps=2 * r * units * 2,
        )

    seconds, dz_pieces, results = [], [], []

    def do_second_norm(i):
        dz, low, result, sums = line(
            functools.partial(second_norm_kernel, i),
            "second_norm",
            [((r, width), F32), ((r, width), BF), ((r, width), BF), ((3, width), F32)],
            [
                *feed_terms[i],
                firsts[i][0],
                *cots,
                *vectors,
            ],
            flops=40 * r * width,
            scratch=[spread, pltpu.VMEM((r, width), F32)],
        )
        seconds.append((dz, sums))
        results.append(result)
        dz_pieces.append(gather_blocks(low))

    backs = {}

    def do_feed_back(i, j):
        backs[i, j] = line(
            feed_back_kernel,
            "feed_back",
            [((2 * r, units), BF), ((r, width), BF), ((r, width), BF), ((1, units), F32)],
            [*dz_pieces[i][2 * j : 2 * j + 2], feeds[i, j][1], w_down, w_in],
            flops=8 * r * width * units,
        )

    thirds, dz1_pieces = [], []

    def do_first_back(i):
        low, sums = line(
            first_back_kernel,
            "first_back",
            [((r, width), BF), ((3, width), F32)],
            [*back_terms[i], seconds[i][0], *firsts[i], *vectors],
            flops=30 * r * width,
            scratch=[spread],
        )
        thirds.append(sums)
        dz1_pieces.append(gather_blocks(low))

    dprojs, token_terms, b_proj_parts = [], [], []

    def do_attend_back(i):
        dproj, keep, send, dz_cols, bias = line(
            attend_back_kernel,
            "attend_back",
            [
                ((LEN, 3 * cols), BF),
                ((2, LEN, cols), BF),
                ((2, LEN, cols), BF),
                ((LEN, cols), BF),
                ((1, 3 * cols), F32),
            ],
            [*dz1_pieces[i], w_out, projs[i], totals[i], labels[i], w_query, w_key, w_value],
            flops=2 * LEN * width * 4 * cols + 10 * LEN * LEN * cols * heads,
            exps=heads * LEN * LEN,
            scratch=[pltpu.VMEM((LEN, cols), BF)],
        )
        token_terms.append((dz_cols, keep, swap(send, "tensor", 1)))
        dprojs.append(dproj)
        b_proj_parts.append(bias)

    def do_tokens_onward(i):
        dz_cols, keep, sent = token_terms[i]
        token_terms[i] = [dz_cols, keep, sent, onward(keep, sent, True)]

    feed_terms, back_terms = {}, {}

    def send_beside(terms, i, b0, b1, b2, b3):
        terms[i] = (b0, swap(b1, "tensor", 1), b2, swap(b3, "tensor", 1))

    def send_across(terms, i):
        b0, near, b2, far = terms[i]
        terms[i] = (b0, near, onward(b2, far, False))

    def staggered(first, second):
        for i in every:
            first(i)
            if i:
                second(i - 1)

    do_attend(0)
    (vectors,) = line(
        vectors_kernel, "vectors", [((6, cols), BF)], [b_out, gain_one, bias_one, b_down, gain_two, bias_two]
    )
    vectors = gather_blocks(vectors)
    cots = exchange_blocks(
        line(
            functools.partial(cot_pack_kernel, count), "cot_pack", [((count * r, cols), BF)] * 4, [cotangent]
        )
    )
    rest_across = line.after(rest_across)
    pieces.append((rest, swap(rest, "tensor", 1), rest_across, swap(rest_across, "tensor", 1)))
    for i in every[1:]:
        do_attend(i)
        do_attend_onward(i - 1)
        if i == 1:
            line.take(*cots, *vectors)
    do_attend_onward(count - 1)

    for i in every:
        do_first_norm(i)
        do_feed(i, 0)

    def second_feed(i):
        do_feed(i, 1)
        send_beside(feed_terms, i, *feeds[i, 0][2:], *feeds[i, 1][2:])

    staggered(second_feed, lambda i: send_across(feed_terms, i))
    send_across(feed_terms, count - 1)
    for i in every:
        do_second_norm(i)
        do_feed_back(i, 0)

    early, late = dp_bits(0), dp_bits(1)

    def second_back(i):
        do_feed_back(i, 1)
        send_beside(back_terms, i, *backs[i, 0][1:3], *backs[i, 1][1:3])

    for i in every[:-1]:
        second_back(i)
        if i:
            send_across(back_terms, i - 1)
    down_pairs = [
        ([feeds[i, j][0]], dz_pieces[i][2 * j : 2 * j + 2]) for i in every for j in range(2)
    ]
    down = Steps(
        dp_sum(line, *weight_grad(line, down_pairs, units, width, early[0], "down_grad"), early, "down")
    )
    for i in every[-2:-1]:
        send_across(back_terms, i)
    second_back(count - 1)
    in_pairs = [
        (h_pieces[i][2 * j : 2 * j + 2], [backs[i, j][0]]) for i in every for j in range(2)
    ]
    into = Steps(
        dp_sum(line, *weight_grad(line, in_pairs, width, units, early[0], "in_grad"), early, "into")
    )
    send_across(back_terms, count - 1)
    for i in every[:-1]:
        do_first_back(i)
    down.go()
    do_first_back(count - 1)
    pieces_out = exchange_blocks(
        line(
            functools.partial(out_pack_kernel, count),
            "out_pack",
            [((count * r, cols), BF)] * 4,
            results,
        )
    )
    wide = exchange_blocks(
        line(
            functools.partial(pack_kernel, count),
            "pack",
            [((6, cols), F32)] * 4,
            [s for _, s in seconds] + thirds,
            scratch=[spread],
        )
    )

    do_attend_back(0)
    down.go()
    into.go()
    do_attend_back(1 % count)
    for i in every[2:]:
        do_attend_back(i)
    down.go()
    into.go()
    out_pairs = [([ctxs[i]], [dz1_pieces[i][k] for k in range(4)]) for i in every]
    out_half = weight_grad(line, out_pairs, width, cols, late[0], "out_grad", stacked=True)
    extra = -(-(6 + units // cols + 3) // 32) * 16
    (packed,) = line(
        functools.partial(small_pack_kernel, count),
        "small_pack",
        [((extra, 2 * cols), BF)],
        [*wide, *[b[3] for b in backs.values()], *b_proj_parts],
    )
    half_shape = ((width // 2, 2 * cols), BF)
    more_shape = ((width // 2 + extra, 2 * cols), BF)
    first_half = line(
        functools.partial(proj_grad_kernel, count, (early[0], early[0], late[0])),
        "proj_grad",
        [half_shape, half_shape, more_shape, more_shape],
        [*pieces[0], *pieces[1], *dprojs, *out_half, packed],
        flops=2 * row_count * width * 3 * cols,
        scratch=[pltpu.VMEM((width, 3 * cols), BF)],
    )
    query_key = Steps(dp_sum(line, first_half[0], first_half[1], early, "query_key", split_kernel(None)))
    small_total = []
    value_out = Steps(
        dp_sum(
            line,
            first_half[2],
            first_half[3],
            late,
            "value_out",
            split_kernel((cols, width)),
            extra,
            small_total,
        )
    )
    down.go()
    into.go()
    for i in every:
        do_tokens_onward(i)
    query_key.go()
    value_out.go()
    down.go()
    into.go()
    query_key.go()
    value_out.go()
    while not small_total:
        value_out.go()
    sums = line(
        small_out_kernel,
        "small_out",
        [((s,), F32) for s in [cols] * 6 + [units] + [cols] * 3],
        small_total,
    )
    into.go()
    (result,) = line(
        functools.partial(rows_kernel, count), "out_rows", [((row_count, cols), BF)], pieces_out
    )
    query_key.go()
    value_out.go()
    (grad_tokens,) = line(
        tokens_kernel, "token_rows", [((row_count, cols), BF)], [x for terms in token_terms for x in terms]
    )
    query_key.go()
    value_out.go()
    down.go()
    query_key.go()
    value_out.go()
    into.go()
    query_key.go()
    value_out.go()
    waiting = [query_key, value_out, into, down]
    while any(s.result is None for s in waiting):
        for s in waiting:
            s.go()
    return (
        result,
        grad_tokens,
        query_key.result[0],
        query_key.result[1],
        value_out.result[0],
        sums[7],
        sums[9],
        value_out.result[1],
        sums[5],
        sums[3],
        sums[4],
        into.result[0],
        sums[6],
        down.result[0],
        sums[2],
        sums[0],
        sums[1],
    )


def solution(mesh):
    placed = (
        P("dp", "tensor"),
        P("dp"),
        P(None, "tensor"),
        P(None, "tensor"),
        P(None, "tensor"),
        P("tensor"),
        P("tensor"),
        P("tensor", None),
        P("tensor"),
        P("tensor"),
        P("tensor"),
        P(None, "tensor"),
        P("tensor"),
        P("tensor", None),
        P("tensor"),
        P("tensor"),
        P("tensor"),
        P("dp", "tensor"),
    )
    return jax.shard_map(
        local,
        mesh=mesh,
        in_specs=placed,
        out_specs=(
            P("dp", "tensor"),
            P("dp", "tensor"),
            P(None, "tensor"),
            P(None, "tensor"),
            P(None, "tensor"),
            P("tensor"),
            P("tensor"),
            P("tensor", None),
            P("tensor"),
            P("tensor"),
            P("tensor"),
            P(None, "tensor"),
            P("tensor"),
            P("tensor", None),
            P("tensor"),
            P("tensor"),
            P("tensor"),
        ),
        check_vma=False,
    )
```

```python
import functools
import math

import jax
import jax.numpy as jnp
from jax import lax
from jax.experimental import pallas as pl
from jax.experimental.pallas import tpu as pltpu
from jax.sharding import PartitionSpec as P

HD = 64
LEN = 512

EPSILON = 1e-05
MASKED = -1000000000.0
VMEM_LIMIT = 8 << 20
BF = jnp.bfloat16
F32 = jnp.float32


def mm(left, right):
    return lax.dot_general(left, right, (((1,), (0,)), ((), ())), preferred_element_type=F32)


def over_rows(left, right):
    return lax.dot_general(left, right, (((0,), (0,)), ((), ())), preferred_element_type=F32)


def against(left, right):
    return lax.dot_general(left, right, (((1,), (1,)), ((), ())), preferred_element_type=F32)


def swap(values, axis, bit):
    size = lax.axis_size(axis)
    return lax.ppermute(values, axis, [(i, i ^ bit) for i in range(size)])


def gather_blocks(own):
    across = swap(own, "tensor", 2)
    beside = swap(own, "tensor", 1)
    corner = swap(across, "tensor", 1)
    return own, beside, across, corner


def exchange_blocks(blocks):
    return (
        blocks[0],
        swap(blocks[1], "tensor", 1),
        swap(blocks[2], "tensor", 2),
        swap(blocks[3], "tensor", 3),
    )


def dp_bits(order):
    size = lax.axis_size("dp")
    bits = [1 << i for i in range(int(math.log2(size)))]
    if order and len(bits) > 1:
        bits[0], bits[1] = bits[1], bits[0]
    return bits


class Line:
    def __init__(self, place):
        self.place = place

    def __call__(self, kernel, name, out_shape, operands, flops=0, exps=0, scratch=()):
        out_shape = [jax.ShapeDtypeStruct(s, d) for s, d in out_shape]
        size = sum(math.prod(o.shape) * o.dtype.itemsize for o in list(operands) + out_shape)
        whole = pl.BlockSpec(memory_space=pltpu.VMEM)
        outs = pl.pallas_call(
            kernel,
            in_specs=[pl.BlockSpec(memory_space=pltpu.SMEM)] + [whole] * len(operands),
            out_specs=[whole] * len(out_shape),
            out_shape=out_shape,
            scratch_shapes=list(scratch),
            compiler_params=pltpu.CompilerParams(vmem_limit_bytes=VMEM_LIMIT),
            cost_estimate=pl.CostEstimate(flops=flops, transcendentals=exps, bytes_accessed=size),
            name=name,
        )(self.place, *operands)
        last = min(outs, key=lambda o: math.prod(o.shape))
        self.place, _ = lax.optimization_barrier((self.place, last))
        return outs

    def after(self, value):
        return lax.optimization_barrier((value, self.place))[0]

    def take(self, *values):
        self.place = lax.optimization_barrier((self.place, *values))[0]


def block(index, size):
    return pl.ds(pl.multiple_of(index * size, size), size)


def first_of(ref):
    return (ref[0] if len(ref.shape) == 3 else ref[...]).astype(F32)


def head_lanes(width, head):
    lane = lax.broadcasted_iota(jnp.int32, (1, width), 1)
    return (lane >= head * HD) & (lane < (head + 1) * HD)


def allowed_block(label_row):
    length = label_row.shape[1]
    label_row = label_row.astype(F32)
    label_column = jnp.transpose(jnp.broadcast_to(label_row, (8, length)))[:, :1]
    same = label_column == label_row
    diagonal = lax.broadcasted_iota(jnp.int32, (length, length), 0) == lax.broadcasted_iota(
        jnp.int32, (length, length), 1
    )
    return same & ((label_column != 0.0) | diagonal)


def attend_kernel(
    sequence, place, p0, p1, p2, p3, wq, wk, wv, bq, bv, label, w_out, proj, ctx, total, residual, keep, send
):
    t = place[0]
    width = wq.shape[1]
    length = ctx.shape[0]
    rows = length // 4
    pieces = [p.at[sequence * length : (sequence + 1) * length, :] for p in (p0, p1, p2, p3)]
    for k, piece in enumerate(pieces):
        residual[:, block(t ^ k, width)] = piece[block(t, rows), :]
    parts = []
    for weight in (wq, wk, wv):
        parts.append(total_of([mm(piece[...], weight[block(t ^ k, width), :]) for k, piece in enumerate(pieces)]))
    queries = (parts[0] + bq[...].astype(F32)[None, :]).astype(BF)
    keys = parts[1].astype(BF)
    values = (parts[2] + bv[...].astype(F32)[None, :]).astype(BF)
    proj[:, :width] = queries
    proj[:, width : 2 * width] = keys
    proj[:, 2 * width :] = values
    allowed = allowed_block(label[...])
    context = jnp.zeros(queries.shape, F32)
    zero = jnp.zeros((), BF)
    for head in range(width // HD):
        lanes = head_lanes(width, head)
        scores = against(jnp.where(lanes, queries, zero), keys) * (HD**-0.5)
        scores = jnp.where(allowed, scores, MASKED)
        peak = jnp.max(scores, axis=1, keepdims=True)
        terms = jnp.exp(scores - peak)
        summed = jnp.sum(terms, axis=1, keepdims=True)
        probs = (terms / summed).astype(BF)
        context = context + mm(probs, jnp.where(lanes, values, zero))
        total[:, head : head + 1] = peak + jnp.log(summed)
    context = context.astype(BF)
    for j in range(4):
        ctx[block(t ^ j, rows), :] = context[j * rows : (j + 1) * rows]
    for k in range(4):
        part = mm(ctx[k * rows : (k + 1) * rows, :], w_out[...]).astype(BF)
        (send if k % 2 else keep)[k // 2] = part


def attend_back_kernel(
    place, d0, d1, d2, d3, w_out, proj, total, label, wq, wk, wv, dproj, keep, send, dz_cols, bias, dctx
):
    t = place[0]
    width = wq.shape[1]
    rows = d0.shape[0]
    for k, piece in enumerate((d0, d1, d2, d3)):
        dctx[block(t ^ k, rows), :] = against(piece[...], w_out[...]).astype(BF)
        dz_cols[block(t ^ k, rows), :] = piece[:, block(t, width)]
    allowed = allowed_block(label[...])
    queries, keys, values = proj[:, :width], proj[:, width : 2 * width], proj[:, 2 * width :]
    dcontext = dctx[...]
    scale = HD**-0.5
    dquery = jnp.zeros(queries.shape, F32)
    dkey = jnp.zeros(queries.shape, F32)
    dvalue = jnp.zeros(queries.shape, F32)
    zero = jnp.zeros((), BF)
    for head in range(width // HD):
        lanes = head_lanes(width, head)
        q_head = jnp.where(lanes, queries, zero)
        d_head = jnp.where(lanes, dcontext, zero)
        k_head = jnp.where(lanes, keys, zero)
        scores = against(q_head, keys) * scale
        scores = jnp.where(allowed, scores, MASKED)
        probs = jnp.exp(scores - total[:, head : head + 1])
        dprobs = against(d_head, values)
        delta = jnp.sum(probs * dprobs, axis=1, keepdims=True)
        dscores = (probs * (dprobs - delta)).astype(BF)
        dquery = dquery + mm(dscores, k_head)
        dkey = dkey + over_rows(dscores, q_head)
        dvalue = dvalue + over_rows(probs.astype(BF), d_head)
    grads = ((dquery * scale).astype(BF), (dkey * scale).astype(BF), dvalue.astype(BF))
    for i, grad in enumerate(grads):
        dproj[:, i * width : (i + 1) * width] = grad
        bias[:, i * width : (i + 1) * width] = jnp.sum(grad.astype(F32), axis=0, keepdims=True)
    for k in range(4):
        here = block(t ^ k, width)
        part = total_of([against(grad, weight[here, :]) for grad, weight in zip(grads, (wq, wk, wv))])
        (send if k % 2 else keep)[k // 2] = part.astype(BF)


def normed_of(values):
    center = values - jnp.mean(values, axis=1, keepdims=True)
    inverse = lax.rsqrt(jnp.mean(center * center, axis=1, keepdims=True) + EPSILON)
    return center * inverse, inverse


def norm_back(scaled, normed, inverse):
    mean = jnp.mean(scaled, axis=1, keepdims=True)
    along = jnp.mean(scaled * normed, axis=1, keepdims=True)
    return inverse * (scaled - mean - normed * along)


def fill(vectors, spread, t):
    width = vectors[0].shape[1]
    for k, ref in enumerate(vectors):
        spread[0:6, block(t ^ k, width)] = ref[...].astype(F32)


def onward_kernel(place, kept, got, out):
    out[...] = (kept[...].astype(F32) + got[...].astype(F32)).astype(BF)


def second_of_onward_kernel(place, kept, got, out):
    out[...] = (kept[1].astype(F32) + got[1].astype(F32)).astype(BF)


def vectors_kernel(place, *refs):
    for i, ref in enumerate(refs[:-1]):
        refs[-1][i : i + 1, :] = ref[...][None, :]


def first_norm_kernel(place, s0, s1, s2, residual, v0, v1, v2, v3, normed_ref, inverse_ref, low, spread):
    fill((v0, v1, v2, v3), spread, place[0])
    z = first_of(s0) + first_of(s1) + first_of(s2)
    z = residual[...].astype(F32) + z + spread[0:1, :]
    normed, inverse = normed_of(z)
    normed_ref[...] = normed
    inverse_ref[...] = inverse
    low[...] = (normed * spread[1:2, :] + spread[2:3, :]).astype(BF)


def cot_pack_kernel(count, place, cot, *outs):
    t = place[0]
    r = outs[0].shape[0] // count
    for k, out in enumerate(outs):
        for i in range(count):
            out[i * r : (i + 1) * r, :] = cot[block(4 * i + (t ^ k), r), :]


def second_norm_kernel(
    sequence, place, s0, s1, s2, normed_one, c0, c1, c2, c3, v0, v1, v2, v3, dz, low, out, sums, spread, cots
):
    t = place[0]
    fill((v0, v1, v2, v3), spread, t)
    width = c0.shape[1]
    r = dz.shape[0]
    for k, ref in enumerate((c0, c1, c2, c3)):
        cots[:, block(t ^ k, width)] = ref[sequence * r : (sequence + 1) * r, :].astype(F32)
    h_one = normed_one[...] * spread[1:2, :] + spread[2:3, :]
    z = h_one + (s0[...].astype(F32) + s1[...].astype(F32) + s2[...].astype(F32)) + spread[3:4, :]
    normed, inverse = normed_of(z)
    out[...] = (normed * spread[4:5, :] + spread[5:6, :]).astype(BF)
    grad = cots[...]
    sums[0:1, :] = jnp.sum(grad * normed, axis=0, keepdims=True)
    sums[1:2, :] = jnp.sum(grad, axis=0, keepdims=True)
    back = norm_back(grad * spread[4:5, :], normed, inverse)
    sums[2:3, :] = jnp.sum(back, axis=0, keepdims=True)
    dz[...] = back
    low[...] = back.astype(BF)


def first_back_kernel(place, s0, s1, s2, dz, normed_ref, inverse_ref, v0, v1, v2, v3, low, sums, spread):
    fill((v0, v1, v2, v3), spread, place[0])
    dh = dz[...] + (s0[...].astype(F32) + s1[...].astype(F32) + s2[...].astype(F32))
    normed = normed_ref[...]
    sums[0:1, :] = jnp.sum(dh * normed, axis=0, keepdims=True)
    sums[1:2, :] = jnp.sum(dh, axis=0, keepdims=True)
    back = norm_back(dh * spread[1:2, :], normed, inverse_ref[...])
    sums[2:3, :] = jnp.sum(back, axis=0, keepdims=True)
    low[...] = back.astype(BF)


def feed_kernel(place, h0, h1, w_in, b_in, w_down, hidden, slope, keep, send):
    rows = jnp.concatenate([h0[...], h1[...]], axis=0)
    r = h0.shape[0]
    units = w_in.shape[1]
    step = min(256, units)
    total = jnp.zeros((2 * r, w_down.shape[1]), F32)
    for first in range(0, units, step):
        here = slice(first, first + step)
        pre_act = mm(rows, w_in[:, here]) + b_in[here].astype(F32)[None, :]
        cdf = 0.5 * (1.0 + lax.erf(pre_act * (2.0**-0.5)))
        rise = pre_act * jnp.exp(-0.5 * pre_act * pre_act) * ((2.0 * math.pi) ** -0.5)
        active = (pre_act * cdf).astype(BF)
        hidden[:, here] = active
        slope[:, here] = (cdf + rise).astype(BF)
        total = total + mm(active, w_down[here, :])
    keep[...] = total[:r].astype(BF)
    send[...] = total[r:].astype(BF)


def feed_back_kernel(place, d0, d1, slope, w_down, w_in, dpre, keep, send, bias):
    rows = jnp.concatenate([d0[...], d1[...]], axis=0)
    r = d0.shape[0]
    units = w_in.shape[1]
    step = min(256, units)
    total = jnp.zeros((2 * r, w_in.shape[0]), F32)
    for first in range(0, units, step):
        here = slice(first, first + step)
        grad = (against(rows, w_down[here, :]) * slope[:, here].astype(F32)).astype(BF)
        dpre[:, here] = grad
        bias[:, here] = jnp.sum(grad.astype(F32), axis=0, keepdims=True)
        total = total + against(grad, w_in[:, here])
    keep[...] = total[:r].astype(BF)
    send[...] = total[r:].astype(BF)


def weight_grad_kernel(groups, stacked, bit, place, *refs):
    keep, send = refs[-2:]
    set_bit = jnp.where((place[1] & bit) == 0, 0, 1)
    lefts, rights = [], []
    at = 0
    for left, right in groups:
        lefts.append(refs[at : at + left])
        rights.append(refs[at + left : at + left + right])
        at += left + right

    def joined(parts, columns):
        parts = [p[:, columns] for p in parts]
        return parts[0] if len(parts) == 1 else jnp.concatenate(parts, axis=0)

    half, width = keep.shape
    step = min(256, half)
    for half_index, out in ((1 - set_bit, send), (set_bit, keep)):
        for first in range(0, half, step):
            here = block(half_index * (half // step) + first // step, step)
            if stacked:
                terms = [over_rows(joined(l, slice(None)), joined(r, here)) for l, r in zip(lefts, rights)]
            else:
                terms = [over_rows(joined(l, here), joined(r, slice(None))) for l, r in zip(lefts, rights)]
            out[first : first + step, :] = total_of(terms).astype(BF)


def weight_grad(line, pairs, height, width, bit, name, stacked=False):
    operands = [x for left, right in pairs for x in (*left, *right)]
    groups = [(len(left), len(right)) for left, right in pairs]
    depth = sum(x.shape[0] for left, _ in pairs for x in left)
    return line(
        functools.partial(weight_grad_kernel, groups, stacked, bit),
        name,
        [((height // 2, width), BF)] * 2,
        operands,
        flops=2 * depth * height * width,
    )


def proj_grad_kernel(count, bits, place, *refs):
    t = place[0]
    out_keep, out_send, packed = refs[8 + count : 11 + count]
    outs, full = refs[-5:-1], refs[-1]
    size = refs[0].shape[1]
    rows = refs[0].shape[0]
    for k in range(4):
        terms = [over_rows(refs[k][...], refs[8][...])]
        for i in range(1, count):
            terms.append(over_rows(refs[4 + k][(i - 1) * rows : i * rows, :], refs[8 + i][...]))
        full[block(t ^ k, size), :] = total_of(terms).astype(BF)
    half = outs[0].shape[0]
    outs[2][half:, :] = packed[...]
    outs[3][half:, :] = packed[...]
    for j, bit in enumerate(bits):
        set_bit = jnp.where((place[1] & bit) == 0, 0, 1)
        columns = slice(j * size, (j + 1) * size)
        to = slice((j % 2) * size, (j % 2 + 1) * size)
        outs[2 * (j // 2)][:half, to] = full[block(set_bit, half), columns]
        outs[2 * (j // 2) + 1][:half, to] = full[block(1 - set_bit, half), columns]
    outs[2][:half, size:] = out_keep[...]
    outs[3][:half, size:] = out_send[...]


def halve_kernel(bit, extra, place, kept, got, keep, send):
    set_bit = jnp.where((place[1] & bit) == 0, 0, 1)
    half = keep.shape[0] - extra
    for index, out in ((1 - set_bit, send), (set_bit, keep)):
        here = block(index, half)
        out[:half, :] = (kept[here, :].astype(F32) + got[here, :].astype(F32)).astype(BF)
        if extra:
            out[half:, :] = (kept[2 * half :, :].astype(F32) + got[2 * half :, :].astype(F32)).astype(BF)


def add_kernel(place, kept, got, out, *rest):
    half = out.shape[0]
    out[...] = (kept[:half, :].astype(F32) + got[:half, :].astype(F32)).astype(BF)
    for ref in rest:
        ref[...] = kept[half:, :].astype(F32) + got[half:, :].astype(F32)


def join_kernel(bit, place, mine, got, out):
    set_bit = jnp.where((place[1] & bit) == 0, 0, 1)
    half = mine.shape[0]
    for index, ref in ((set_bit, mine), (1 - set_bit, got)):
        out[block(index, half), :] = ref[...].astype(out.dtype)


def split_kernel(unstack):
    def shapes(height, width):
        return [((height, width // 2), F32), (unstack or (height, width // 2), F32)]

    def kernel(bit, place, mine, got, one, two):
        set_bit = jnp.where((place[1] & bit) == 0, 0, 1)
        half = mine.shape[0]
        size = one.shape[1]
        for index, ref in ((set_bit, mine), (1 - set_bit, got)):
            one[block(index, half), :] = ref[:, :size].astype(F32)
            if unstack:
                tall = unstack[0]
                for j in range(half // tall):
                    columns = block(index * (half // tall) + j, size)
                    two[:, columns] = ref[j * tall : (j + 1) * tall, size:].astype(F32)
            else:
                two[block(index, half), :] = ref[:, size:].astype(F32)

    return shapes, kernel


def whole_shapes(height, width):
    return [((height, width), F32)]


def dp_sum(line, keep, send, bits, name, last=(whole_shapes, join_kernel), extra=0, rests=()):
    got = swap(send, "dp", bits[0])
    yield
    half, width = keep.shape
    half -= extra
    for bit in bits[1:]:
        half //= 2
        keep, send = line(
            functools.partial(halve_kernel, bit, extra),
            name + "_halve",
            [((half + extra, width), BF)] * 2,
            [keep, got],
        )
        got = swap(send, "dp", bit)
        yield
    mine, *rest = line(
        add_kernel, name + "_add", [((half, width), BF)] + [((extra, width), F32)] * (extra > 0), [keep, got]
    )
    if extra:
        rests.extend(rest)
    got = swap(mine, "dp", bits[-1])
    yield
    for bit in reversed(bits[1:]):
        half *= 2
        (mine,) = line(
            functools.partial(join_kernel, bit), name + "_join", [((half, width), BF)], [mine, got]
        )
        got = swap(mine, "dp", bits[bits.index(bit) - 1])
        yield
    shapes, kernel = last
    return line(
        functools.partial(kernel, bits[0]), name + "_whole", shapes(2 * half, width), [mine, got]
    )


class Steps:
    def __init__(self, generator):
        self.generator = generator
        self.result = None
        self.go()

    def go(self, times=1):
        for _ in range(times):
            if self.result is None:
                try:
                    next(self.generator)
                except StopIteration as stop:
                    self.result = stop.value

    def finish(self):
        while self.result is None:
            self.go()
        return self.result


def small_pack_kernel(count, place, *refs):
    out = refs[-1]
    width = out.shape[1] // 2
    b_in = total_of([ref[...] for ref in refs[4 : 4 + 2 * count]])
    b_proj = total_of([ref[...] for ref in refs[4 + 2 * count : 4 + 3 * count]])
    features = total_of([ref[...] for ref in refs[:4]])
    rows = [features[i : i + 1, :] for i in range(6)]
    for whole in (b_in, b_proj):
        rows += [whole[:, j * width : (j + 1) * width] for j in range(whole.shape[1] // width)]
    rows += [jnp.zeros((1, width), F32)] * (2 * out.shape[0] - len(rows))
    left, right = jnp.concatenate(rows[0::2], axis=0), jnp.concatenate(rows[1::2], axis=0)
    out[...] = jnp.concatenate([left, right], axis=1).astype(BF)


def small_out_kernel(place, total, *outs):
    width = total.shape[1] // 2
    row = 0
    for out in outs:
        for j in range(out.shape[0] // width):
            out[j * width : (j + 1) * width] = total[row // 2, (row % 2) * width : (row % 2 + 1) * width]
            row += 1


def out_pack_kernel(count, place, *refs):
    t = place[0]
    r = refs[0].shape[0]
    for k, out in enumerate(refs[count:]):
        for i in range(count):
            out[i * r : (i + 1) * r, :] = refs[i][:, block(t ^ k, out.shape[1])]


def rows_kernel(count, place, *refs):
    t = place[0]
    out = refs[-1]
    r = refs[0].shape[0] // count
    for k in range(4):
        for i in range(count):
            out[block(4 * i + (t ^ k), r), :] = refs[k][i * r : (i + 1) * r, :]


def tokens_kernel(place, *refs):
    out = refs[-1]
    r = refs[0].shape[0]
    for i in range((len(refs) - 1) // 4):
        terms = [first_of(refs[4 * i + j]) for j in range(4)]
        out[i * r : (i + 1) * r, :] = total_of(terms).astype(BF)


def pack_kernel(count, place, *refs):
    t = place[0]
    outs, spread = refs[2 * count : 2 * count + 4], refs[-1]
    spread[0:3, :] = total_of([refs[i][...] for i in range(count)])
    spread[3:6, :] = total_of([refs[count + i][...] for i in range(count)])
    width = outs[0].shape[1]
    for k, ref in enumerate(outs):
        ref[...] = spread[0:6, block(t ^ k, width)]


def total_of(parts):
    return functools.reduce(lambda a, b: a + b, parts)


def local(
    tokens,
    segment_ids,
    w_query,
    w_key,
    w_value,
    b_query,
    b_value,
    w_out,
    b_out,
    gain_one,
    bias_one,
    w_in,
    b_in,
    w_down,
    b_down,
    gain_two,
    bias_two,
    cotangent,
):
    t = lax.axis_index("tensor")
    d = lax.axis_index("dp")
    line = Line(jnp.stack([t, d]).astype(jnp.int32))
    row_count, cols = tokens.shape
    width = w_query.shape[0]
    units = w_in.shape[1]
    count = row_count // LEN
    r = LEN // 4
    heads = cols // HD
    labels = segment_ids.reshape(count, 1, LEN)
    every = range(count)
    spread = pltpu.VMEM((8, width), F32)

    first, rest = tokens[:LEN], tokens[LEN:]
    rest_across = swap(rest, "tensor", 2)
    pieces = [gather_blocks(first)]

    def onward(kept, got, pair):
        (both,) = line(
            second_of_onward_kernel if pair else onward_kernel,
            "onward",
            [(kept.shape[1:] if pair else kept.shape, BF)],
            [kept, got],
        )
        return swap(both, "tensor", 2)

    ctxs, projs, totals, attn_terms = [], [], [], []

    def do_attend(i):
        proj, ctx, total, residual, keep, send = line(
            functools.partial(attend_kernel, max(i - 1, 0)),
            "attend",
            [
                ((LEN, 3 * cols), BF),
                ((LEN, cols), BF),
                ((LEN, heads), F32),
                ((r, width), BF),
                ((2, r, width), BF),
                ((2, r, width), BF),
            ],
            [*pieces[min(i, 1)], w_query, w_key, w_value, b_query, b_value, labels[i], w_out],
            flops=2 * LEN * width * 4 * cols + 4 * LEN * LEN * cols * heads,
            exps=heads * LEN * LEN,
        )
        attn_terms.append((keep, swap(send, "tensor", 1), residual))
        projs.append(proj)
        ctxs.append(ctx)
        totals.append(total)

    def do_attend_onward(i):
        keep, sent, residual = attn_terms[i]
        attn_terms[i] = [keep, sent, onward(keep, sent, True), residual]

    firsts, h_pieces = [], []

    def do_first_norm(i):
        normed, inverse, low = line(
            first_norm_kernel,
            "first_norm",
            [((r, width), F32), ((r, 1), F32), ((r, width), BF)],
            [*attn_terms[i], *vectors],
            flops=20 * r * width,
            scratch=[spread],
        )
        firsts.append((normed, inverse))
        h_pieces.append(gather_blocks(low))

    feeds = {}

    def do_feed(i, j):
        feeds[i, j] = line(
            feed_kernel,
            "feed",
            [((2 * r, units), BF), ((2 * r, units), BF), ((r, width), BF), ((r, width), BF)],
            [*h_pieces[i][2 * j : 2 * j + 2], w_in, b_in, w_down],
            flops=8 * r * width * units,
            exps=2 * r * units * 2,
        )

    seconds, dz_pieces, results = [], [], []

    def do_second_norm(i):
        dz, low, result, sums = line(
            functools.partial(second_norm_kernel, i),
            "second_norm",
            [((r, width), F32), ((r, width), BF), ((r, width), BF), ((3, width), F32)],
            [
                *feed_terms[i],
                firsts[i][0],
                *cots,
                *vectors,
            ],
            flops=40 * r * width,
            scratch=[spread, pltpu.VMEM((r, width), F32)],
        )
        seconds.append((dz, sums))
        results.append(result)
        dz_pieces.append(gather_blocks(low))

    backs = {}

    def do_feed_back(i, j):
        backs[i, j] = line(
            feed_back_kernel,
            "feed_back",
            [((2 * r, units), BF), ((r, width), BF), ((r, width), BF), ((1, units), F32)],
            [*dz_pieces[i][2 * j : 2 * j + 2], feeds[i, j][1], w_down, w_in],
            flops=8 * r * width * units,
        )

    thirds, dz1_pieces = [], []

    def do_first_back(i):
        low, sums = line(
            first_back_kernel,
            "first_back",
            [((r, width), BF), ((3, width), F32)],
            [*back_terms[i], seconds[i][0], *firsts[i], *vectors],
            flops=30 * r * width,
            scratch=[spread],
        )
        thirds.append(sums)
        dz1_pieces.append(gather_blocks(low))

    dprojs, token_terms, b_proj_parts = [], [], []

    def do_attend_back(i):
        dproj, keep, send, dz_cols, bias = line(
            attend_back_kernel,
            "attend_back",
            [
                ((LEN, 3 * cols), BF),
                ((2, LEN, cols), BF),
                ((2, LEN, cols), BF),
                ((LEN, cols), BF),
                ((1, 3 * cols), F32),
            ],
            [*dz1_pieces[i], w_out, projs[i], totals[i], labels[i], w_query, w_key, w_value],
            flops=2 * LEN * width * 4 * cols + 10 * LEN * LEN * cols * heads,
            exps=heads * LEN * LEN,
            scratch=[pltpu.VMEM((LEN, cols), BF)],
        )
        token_terms.append((dz_cols, keep, swap(send, "tensor", 1)))
        dprojs.append(dproj)
        b_proj_parts.append(bias)

    def do_tokens_onward(i):
        dz_cols, keep, sent = token_terms[i]
        token_terms[i] = [dz_cols, keep, sent, onward(keep, sent, True)]

    feed_terms, back_terms = {}, {}

    def send_beside(terms, i, b0, b1, b2, b3):
        terms[i] = (b0, swap(b1, "tensor", 1), b2, swap(b3, "tensor", 1))

    def send_across(terms, i):
        b0, near, b2, far = terms[i]
        terms[i] = (b0, near, onward(b2, far, False))

    def staggered(first, second):
        for i in every:
            first(i)
            if i:
                second(i - 1)

    do_attend(0)
    (vectors,) = line(
        vectors_kernel, "vectors", [((6, cols), BF)], [b_out, gain_one, bias_one, b_down, gain_two, bias_two]
    )
    vectors = gather_blocks(vectors)
    cots = exchange_blocks(
        line(
            functools.partial(cot_pack_kernel, count), "cot_pack", [((count * r, cols), BF)] * 4, [cotangent]
        )
    )
    rest_across = line.after(rest_across)
    pieces.append((rest, swap(rest, "tensor", 1), rest_across, swap(rest_across, "tensor", 1)))
    for i in every[1:]:
        do_attend(i)
        do_attend_onward(i - 1)
        if i == 1:
            line.take(*cots, *vectors)
    do_attend_onward(count - 1)

    for i in every:
        do_first_norm(i)
        do_feed(i, 0)

    def second_feed(i):
        do_feed(i, 1)
        send_beside(feed_terms, i, *feeds[i, 0][2:], *feeds[i, 1][2:])

    staggered(second_feed, lambda i: send_across(feed_terms, i))
    send_across(feed_terms, count - 1)
    for i in every:
        do_second_norm(i)
        do_feed_back(i, 0)

    early, late = dp_bits(0), dp_bits(1)

    def second_back(i):
        do_feed_back(i, 1)
        send_beside(back_terms, i, *backs[i, 0][1:3], *backs[i, 1][1:3])

    for i in every[:-1]:
        second_back(i)
        if i:
            send_across(back_terms, i - 1)
    down_pairs = [
        ([feeds[i, j][0]], dz_pieces[i][2 * j : 2 * j + 2]) for i in every for j in range(2)
    ]
    down = Steps(
        dp_sum(line, *weight_grad(line, down_pairs, units, width, early[0], "down_grad"), early, "down")
    )
    for i in every[-2:-1]:
        send_across(back_terms, i)
    second_back(count - 1)
    in_pairs = [
        (h_pieces[i][2 * j : 2 * j + 2], [backs[i, j][0]]) for i in every for j in range(2)
    ]
    into = Steps(
        dp_sum(line, *weight_grad(line, in_pairs, width, units, early[0], "in_grad"), early, "into")
    )
    send_across(back_terms, count - 1)
    for i in every[:-1]:
        do_first_back(i)
    down.go()
    do_first_back(count - 1)
    pieces_out = exchange_blocks(
        line(
            functools.partial(out_pack_kernel, count),
            "out_pack",
            [((count * r, cols), BF)] * 4,
            results,
        )
    )
    wide = exchange_blocks(
        line(
            functools.partial(pack_kernel, count),
            "pack",
            [((6, cols), F32)] * 4,
            [s for _, s in seconds] + thirds,
            scratch=[spread],
        )
    )

    do_attend_back(0)
    down.go()
    into.go()
    do_attend_back(1 % count)
    for i in every[2:]:
        do_attend_back(i)
    out_pairs = [([ctxs[i]], [dz1_pieces[i][k] for k in range(4)]) for i in every]
    out_half = weight_grad(line, out_pairs, width, cols, late[0], "out_grad", stacked=True)
    extra = -(-(6 + units // cols + 3) // 32) * 16
    (packed,) = line(
        functools.partial(small_pack_kernel, count),
        "small_pack",
        [((extra, 2 * cols), BF)],
        [*wide, *[b[3] for b in backs.values()], *b_proj_parts],
    )
    down.go()
    into.go()
    half_shape = ((width // 2, 2 * cols), BF)
    more_shape = ((width // 2 + extra, 2 * cols), BF)
    first_half = line(
        functools.partial(proj_grad_kernel, count, (early[0], early[0], late[0])),
        "proj_grad",
        [half_shape, half_shape, more_shape, more_shape],
        [*pieces[0], *pieces[1], *dprojs, *out_half, packed],
        flops=2 * row_count * width * 3 * cols,
        scratch=[pltpu.VMEM((width, 3 * cols), BF)],
    )
    query_key = Steps(dp_sum(line, first_half[0], first_half[1], early, "query_key", split_kernel(None)))
    small_total = []
    value_out = Steps(
        dp_sum(
            line,
            first_half[2],
            first_half[3],
            late,
            "value_out",
            split_kernel((cols, width)),
            extra,
            small_total,
        )
    )
    down.go()
    into.go()
    for i in every:
        do_tokens_onward(i)
    query_key.go()
    value_out.go()
    down.go()
    into.go()
    query_key.go()
    value_out.go()
    while not small_total:
        value_out.go()
    sums = line(
        small_out_kernel,
        "small_out",
        [((s,), F32) for s in [cols] * 6 + [units] + [cols] * 3],
        small_total,
    )
    into.go()
    (result,) = line(
        functools.partial(rows_kernel, count), "out_rows", [((row_count, cols), BF)], pieces_out
    )
    query_key.go()
    value_out.go()
    (grad_tokens,) = line(
        tokens_kernel, "token_rows", [((row_count, cols), BF)], [x for terms in token_terms for x in terms]
    )
    query_key.go()
    value_out.go()
    down.go()
    query_key.go()
    value_out.go()
    into.go()
    query_key.go()
    value_out.go()
    waiting = [query_key, value_out, into, down]
    while any(s.result is None for s in waiting):
        for s in waiting:
            s.go()
    return (
        result,
        grad_tokens,
        query_key.result[0],
        query_key.result[1],
        value_out.result[0],
        sums[7],
        sums[9],
        value_out.result[1],
        sums[5],
        sums[3],
        sums[4],
        into.result[0],
        sums[6],
        down.result[0],
        sums[2],
        sums[0],
        sums[1],
    )


def solution(mesh):
    placed = (
        P("dp", "tensor"),
        P("dp"),
        P(None, "tensor"),
        P(None, "tensor"),
        P(None, "tensor"),
        P("tensor"),
        P("tensor"),
        P("tensor", None),
        P("tensor"),
        P("tensor"),
        P("tensor"),
        P(None, "tensor"),
        P("tensor"),
        P("tensor", None),
        P("tensor"),
        P("tensor"),
        P("tensor"),
        P("dp", "tensor"),
    )
    return jax.shard_map(
        local,
        mesh=mesh,
        in_specs=placed,
        out_specs=(
            P("dp", "tensor"),
            P("dp", "tensor"),
            P(None, "tensor"),
            P(None, "tensor"),
            P(None, "tensor"),
            P("tensor"),
            P("tensor"),
            P("tensor", None),
            P("tensor"),
            P("tensor"),
            P("tensor"),
            P(None, "tensor"),
            P("tensor"),
            P("tensor", None),
            P("tensor"),
            P("tensor"),
            P("tensor"),
        ),
        check_vma=False,
    )
```
